32 devices in a mesh: rep: 4 (over x, y), dp: 8 (over z, core).
Axes of the slice: x: 2, y: 2, z: 4, core: 2. Of those that a mesh axis runs over, the one named last changes fastest.
Arguments:
- x: bfloat16 [32, 2048, 768], P(('rep', 'dp')), parts along dimension 0
- dy: bfloat16 [32, 2048, 768], P(('rep', 'dp')), parts along dimension 0
- w_gate: bfloat16 [2, 768, 1792], replicated
- w_up: bfloat16 [2, 768, 1792], replicated
- w_down: bfloat16 [2, 1792, 768], replicated
- m_w_gate: float32 [2, 768, 1792], P(None, 'dp')
- m_w_up: float32 [2, 768, 1792], P(None, 'dp')
- m_w_down: float32 [2, 1792, 768], P(None, 'dp')
- v_w_gate: float32 [2, 768, 1792], P(None, 'dp')
- v_w_up: float32 [2, 768, 1792], P(None, 'dp')
- v_w_down: float32 [2, 1792, 768], P(None, 'dp')
Outputs:
- output 1: bfloat16 [8, 768, 1792], P('rep'), parts along dimension 0
- output 2: bfloat16 [8, 768, 1792], P('rep'), parts along dimension 0
- output 3: bfloat16 [8, 1792, 768], P('rep'), parts along dimension 0
- output 4: float32 [8, 768, 1792], P('rep', 'dp'), parts along dimension 0
- output 5: float32 [8, 768, 1792], P('rep', 'dp'), parts along dimension 0
- output 6: float32 [8, 1792, 768], P('rep', 'dp'), parts along dimension 0
- output 7: float32 [8, 768, 1792], P('rep', 'dp'), parts along dimension 0
- output 8: float32 [8, 768, 1792], P('rep', 'dp'), parts along dimension 0
- output 9: float32 [8, 1792, 768], P('rep', 'dp'), parts along dimension 0
There are 4 independent parts. The reference program is written for one: setup_inputs(seed, part) draws one part's arguments, and reference() takes and returns one part's arrays. A program takes and returns all parts, laid end to end along the dimension named above; an argument that names none is the same for every part.
All inputs are finite; a program needn't handle non-finite values.
Results may differ from the reference program's by a relative error of at most 0.022.
Values are sent between devices in bfloat16 or wider.
A program may use at most 2 GiB of HBM per device.

```python
import jax
import jax.numpy as jnp
from jax import lax

SEQUENCES = 8
TOKENS = 2048
D = 768
FF = 1792
LAYERS = 2
NAMES = ("w_gate", "w_up", "w_down")
SHAPES = {"w_gate": (LAYERS, D, FF), "w_up": (LAYERS, D, FF), "w_down": (LAYERS, FF, D)}


def bump(key, n, height):
    away = (jnp.arange(n, dtype=jnp.int32) - jax.random.randint(key, (), 0, n, jnp.int32)) % n
    return jnp.where(away < n // 8, height, 1.0)


def together(key, own, strength):
    shared = jax.random.normal(key, own.shape[1:], jnp.float32)
    return (own + strength * shared) * lax.rsqrt(1 + strength * strength)


def setup_inputs(seed: int = 0, part: int = 0) -> dict:
    kx, kdy, ka, kb, kz, kf, kh, kl, *keys = jax.random.split(jax.random.key(seed), 8 + 3 * len(NAMES))
    kx, kdy, ka, kb = (jax.random.fold_in(k, part) for k in (kx, kdy, ka, kb))
    kw, km, kv = (keys[i::3] for i in range(3))
    shape = (SEQUENCES, TOKENS, D)
    much_x, much_dy = jax.random.uniform(kz, (2,), jnp.float32, 0.0, 1.0)
    loud = 2.0 ** jax.random.uniform(jax.random.fold_in(kz, 1), (), jnp.float32, -1.0, 2.0)
    layers = 2.0 ** jax.random.uniform(kl, (LAYERS, 1, 1), jnp.float32, -1.0, 1.0)
    x = together(ka, jax.random.normal(kx, shape, jnp.float32), much_x) * bump(kf, D, 4.0)
    dy = together(kb, jax.random.normal(kdy, shape, jnp.float32), much_dy)
    drawn = {"x": x.astype(jnp.bfloat16), "dy": (loud * dy * (SEQUENCES * TOKENS) ** -0.5).astype(jnp.bfloat16)}
    for key, name in zip(kw, NAMES, strict=True):
        w = jax.random.normal(key, SHAPES[name], jnp.float32) * SHAPES[name][1] ** -0.5
        drawn[name] = (w * {"w_gate": 1.0, "w_up": bump(kh, FF, 4.0), "w_down": layers}[name]).astype(jnp.bfloat16)
    for key, name in zip(km, NAMES, strict=True):
        drawn[f"m_{name}"] = 0.1 * jax.random.normal(key, SHAPES[name], jnp.float32)
    for key, name in zip(kv, NAMES, strict=True):
        drawn[f"v_{name}"] = jax.random.uniform(key, SHAPES[name], jnp.float32, 0.005, 0.015)
    return drawn


def matmul(a, w):
    return jnp.dot(a, w, preferred_element_type=jnp.float32).astype(jnp.bfloat16)


def normed(h):
    wide = h.astype(jnp.float32)
    scale = lax.rsqrt(jnp.mean(wide**2, -1, keepdims=True) + 1e-6)
    return (wide * scale).astype(jnp.bfloat16)


def layer(h, w):
    a = normed(h)
    gate = jnp.dot(a, w["w_gate"], preferred_element_type=jnp.float32)
    up = jnp.dot(a, w["w_up"], preferred_element_type=jnp.float32)
    return h + matmul((jax.nn.silu(gate) * up).astype(jnp.bfloat16), w["w_down"])


def adamw(w, m, v, g):
    m = 0.9 * m + 0.1 * g
    v = 0.95 * v + 0.05 * g * g
    step = m * lax.rsqrt(v + 1e-8) + 0.1 * w
    return (w - 0.02 * step).astype(jnp.bfloat16), m, v


def clipped(gradients, sum_of_squares, count):
    factor = jnp.minimum(1.0, 0.5 * lax.rsqrt(sum_of_squares / count + 1e-30))
    return [g * factor for g in gradients]


def stack(weights, h):
    return lax.scan(lambda h, w: (layer(h, w), None), h, weights)[0]


def reference(x, dy, w_gate, w_up, w_down, m_w_gate, m_w_up, m_w_down, v_w_gate, v_w_up, v_w_down):
    weights = dict(zip(NAMES, (w_gate, w_up, w_down), strict=True))

    def take(so_far, sequence):
        h, by_y = sequence
        _, back = jax.vjp(lambda w: stack(w, h), weights)
        return jax.tree.map(lambda total, term: total + term.astype(jnp.float32), so_far, back(by_y)[0]), None

    none_yet = {name: jnp.zeros(w.shape, jnp.float32) for name, w in weights.items()}
    by_weights, _ = lax.scan(take, none_yet, (x, dy))
    gradients = [by_weights[name].astype(jnp.bfloat16).astype(jnp.float32) for name in NAMES]
    gradients = clipped(gradients, sum(jnp.sum(g * g) for g in gradients), sum(g.size for g in gradients))
    new = [
        adamw(w.astype(jnp.float32), m, v, g)
        for w, m, v, g in zip((w_gate, w_up, w_down), (m_w_gate, m_w_up, m_w_down), (v_w_gate, v_w_up, v_w_down), gradients, strict=True)
    ]
    return tuple(one[which] for which in range(3) for one in new)
```

```python
import functools

import jax
import jax.numpy as jnp
from jax import lax
from jax.experimental import pallas as pl
from jax.experimental.pallas import tpu as pltpu
from jax.sharding import PartitionSpec as P

F32, BF16 = jnp.float32, jnp.bfloat16
MESH = pl.DeviceIdType.MESH
VMEM_LIMIT = 67_043_328
CHUNK = 256


def dot(a, b, ca=1, cb=0):
    return lax.dot_general(a, b, (((ca,), (cb,)), ((), ())), preferred_element_type=F32)


def placed():
    me = lax.axis_index("dp")
    z, c = me // 2, me % 2
    h = z // 2
    end = (z + h) % 2 == 0
    return me, z, c, h, end


def remote(src, dst, send, recv, to):
    return pltpu.make_async_remote_copy(
        src_ref=src, dst_ref=dst, send_sem=send, recv_sem=recv, device_id={"dp": to}, device_id_type=MESH
    )


def gradients_kernel(
    T, D, FF, x_hbm, dy_hbm, wg_hbm, wu_hbm, wd_hbm, gg_ref, gu_ref, gd_ref,
    H, A0, A1, AT, DY, ACC, hid, dg, du, wgs, wus, wds,
    own, prec, fin, RE, RM, ownd, precd, find, REd, RMd,
    w_sem, in_sem, d_send, d_recv, e_send, e_recv, m_send, m_recv,
    dd_send, dd_recv, ed_send, ed_recv, md_send, md_recv,
):
    me, z, c, h, end = placed()
    partner = z * 2 + 1 - c
    d = 1 - 2 * h
    inward, outward = (z + d) * 2 + c, (z - d) * 2 + c
    mid = jnp.logical_not(end)
    TT = min(512, T)
    tiles = T // TT
    steps = FF // CHUNK
    RG, RD = D // 8, FF // 8

    def target(q):
        return q + h * (3 - 2 * q)

    def column(i):
        return (i + steps - 2) % steps

    def rows(t):
        return pl.ds(pl.multiple_of(t * TT, TT), TT)

    def weights(l, i, s):
        cols = pl.ds(pl.multiple_of(column(i) * CHUNK, CHUNK), CHUNK)
        slot = s % 2
        return (
            pltpu.make_async_copy(wg_hbm.at[l, :, cols], wgs.at[slot], w_sem.at[slot, 0]),
            pltpu.make_async_copy(wu_hbm.at[l, :, cols], wus.at[slot], w_sem.at[slot, 1]),
            pltpu.make_async_copy(wd_hbm.at[l, cols, :], wds.at[slot], w_sem.at[slot, 2]),
        )

    get_x = pltpu.make_async_copy(x_hbm, H, in_sem.at[0])
    get_dy = pltpu.make_async_copy(dy_hbm, DY, in_sem.at[1])
    get_x.start()
    for copy in weights(0, 0, 0):
        copy.start()
    get_dy.start()

    barrier = pltpu.get_barrier_semaphore()
    pl.semaphore_signal(barrier, inc=1, device_id={"dp": partner}, device_id_type=MESH)
    pl.semaphore_signal(barrier, inc=1, device_id={"dp": inward}, device_id_type=MESH)

    @pl.when(mid)
    def _():
        pl.semaphore_signal(barrier, inc=1, device_id={"dp": outward}, device_id_type=MESH)
        pl.semaphore_wait(barrier, 3)

    @pl.when(end)
    def _():
        pl.semaphore_wait(barrier, 2)

    def normed(wide):
        return wide * lax.rsqrt(jnp.mean(wide * wide, -1, keepdims=True) + 1e-6)

    get_x.wait()

    def first(t, _):
        A0[rows(t)] = normed(H[rows(t)].astype(F32)).astype(BF16)
        return 0

    lax.fori_loop(0, tiles, first, 0)

    def next_weights(l, i, s, after):
        for copy in weights(l, i, s):
            copy.wait()

        @pl.when(i < steps - 1)
        def _():
            for copy in weights(l, i + 1, s + 1):
                copy.start()

        if after is not None:

            @pl.when(i == steps - 1)
            def _():
                for copy in weights(after, 0, s + 1):
                    copy.start()

    def forward(i, _):
        next_weights(0, i, i, 1)
        slot = i % 2

        def tile(t, _):
            a = A0[rows(t)]
            gate, up = dot(a, wgs[slot]), dot(a, wus[slot])
            hidden = (gate * lax.logistic(gate) * up).astype(BF16)
            down = dot(hidden, wds[slot])

            @pl.when(i == 0)
            def _():
                ACC[rows(t)] = down

            @pl.when(i > 0)
            def _():
                ACC[rows(t)] += down

            return 0

        lax.fori_loop(0, tiles, tile, 0)
        return 0

    lax.fori_loop(0, steps, forward, 0)

    def between(t, _):
        out = ACC[rows(t)].astype(BF16).astype(F32)
        h1 = (H[rows(t)].astype(F32) + out).astype(BF16)
        H[rows(t)] = h1
        a = normed(h1.astype(F32)).astype(BF16)
        A1[rows(t)] = a
        AT[:, rows(t)] = a.T
        return 0

    lax.fori_loop(0, tiles, between, 0)
    get_dy.wait()

    def to_partner(k):
        return remote(own.at[k % 4, :, 1 - c], prec.at[k], d_send.at[k], d_recv.at[k], partner)

    def to_partner_d(p, zt):
        block = pl.ds(pl.multiple_of((2 * zt + 1 - c) * RD, RD), RD)
        return remote(ownd.at[p, block], precd.at[p, zt], dd_send.at[p, zt], dd_recv.at[p, zt], partner)

    def from_end(k, q):
        return remote(prec.at[k, target(q)], RE.at[k, q - 1], e_send.at[k, q - 1], e_recv.at[k, q - 1], inward)

    def across(k, q):
        return remote(prec.at[k, target(q)], RM.at[k, 3 - q], e_send.at[k, q - 1], m_recv.at[k, 3 - q], inward)

    def to_end(k):
        return remote(prec.at[k, target(0)], RM.at[k, 0], m_send.at[k], m_recv.at[k, 0], outward)

    def from_end_d(p, q):
        return remote(precd.at[p, target(q)], REd.at[p, q - 1], ed_send.at[p, q - 1], ed_recv.at[p, q - 1], inward)

    def across_d(p, q):
        return remote(precd.at[p, target(q)], RMd.at[p, 3 - q], ed_send.at[p, q - 1], md_recv.at[p, 3 - q], inward)

    def to_end_d(p):
        return remote(precd.at[p, target(0)], RMd.at[p, 0], md_send.at[p], md_recv.at[p, 0], outward)

    def both(k, zt):
        return own[k % 4, zt, c].astype(F32) + prec[k, zt].astype(F32)

    def both_d(p, zt):
        block = pl.ds(pl.multiple_of((2 * zt + c) * RD, RD), RD)
        return ownd[p, block].astype(F32) + precd[p, zt].astype(F32)

    def share(k):
        to_partner(k).wait()
        fin[k] = both(k, z)

        @pl.when(end)
        def _():
            for q in (3, 2, 1):
                prec[k, target(q)] = both(k, target(q)).astype(BF16)
                from_end(k, q).start()

    def share_d(p, zt):
        to_partner_d(p, zt).wait()
        q = zt + h * (3 - 2 * zt)

        @pl.when(zt == z)
        def _():
            find[p] = both_d(p, zt)

        @pl.when(jnp.logical_and(end, zt != z))
        def _():
            precd[p, zt] = both_d(p, zt).astype(BF16)
            from_end_d(p, q).start()

    def pass_on(k):
        @pl.when(mid)
        def _():
            for q in (3, 2):
                from_end(k, q).wait_recv()
                prec[k, target(q)] = (both(k, target(q)) + RE[k, q - 1].astype(F32)).astype(BF16)
                across(k, q).start()

    def pass_back(k):
        @pl.when(mid)
        def _():
            across(k, 3).wait_recv()
            prec[k, target(0)] = (both(k, target(0)) + RM[k, 0].astype(F32)).astype(BF16)
            to_end(k).start()

    def pass_on_d(p, q):
        @pl.when(mid)
        def _():
            from_end_d(p, q).wait_recv()
            precd[p, target(q)] = (both_d(p, target(q)) + REd[p, q - 1].astype(F32)).astype(BF16)
            across_d(p, q).start()

    def pass_back_d(p):
        @pl.when(mid)
        def _():
            across_d(p, 3).wait_recv()
            precd[p, target(0)] = (both_d(p, target(0)) + RMd[p, 0].astype(F32)).astype(BF16)
            to_end_d(p).start()

    def backward(p, A, i, _):
        l = 1 - p
        s = steps * (1 + p) + i
        k = steps * p + i
        slot = s % 2
        j = column(i)
        next_weights(l, i, s, 0 if p == 0 else None)

        def tile(t, _):
            a = A[rows(t)]
            gate, up = dot(a, wgs[slot]), dot(a, wus[slot])
            dh = dot(DY[rows(t)], wds[slot], 1, 1).astype(BF16).astype(F32)
            sig = lax.logistic(gate)
            act = gate * sig
            hid[rows(t)] = (act * up).astype(BF16)
            du[rows(t)] = (dh * act).astype(BF16)
            dg[rows(t)] = (dh * up * (sig * (1.0 + gate * (1.0 - sig)))).astype(BF16)
            return 0

        lax.fori_loop(0, tiles, tile, 0)
        here = pl.ds(pl.multiple_of(j * CHUNK, CHUNK), CHUNK)
        ownd[p, here] = dot(hid[...], DY[...], 0, 0).astype(BF16)
        zt = (i // 2 + 3) % 4
        down_ready = jnp.logical_or(i % 2 == 1, i == steps - 1)

        @pl.when(down_ready)
        def _():
            to_partner_d(p, zt).start()

        own[k % 4, :, :, 0] = dot(AT[...], dg[...]).astype(BF16).reshape(4, 2, RG, CHUNK)
        own[k % 4, :, :, 1] = dot(AT[...], du[...]).astype(BF16).reshape(4, 2, RG, CHUNK)
        to_partner(k).start()

        if p == 0:

            def back(t, _):
                da = dot(dg[rows(t)], wgs[slot], 1, 1) + dot(du[rows(t)], wus[slot], 1, 1)

                @pl.when(i == 0)
                def _():
                    ACC[rows(t)] = da

                @pl.when(i > 0)
                def _():
                    ACC[rows(t)] += da

                return 0

            lax.fori_loop(0, tiles, back, 0)

        @pl.when(down_ready)
        def _():
            share_d(p, zt)

        share(k)

        @pl.when(k >= 2)
        def _():
            pass_on(k - 2)

        @pl.when(k >= 3)
        def _():
            pass_back(k - 3)

        if p == 1:

            @pl.when(i == 3)
            def _():
                pass_on_d(0, 3)
                pass_on_d(0, 2)
                pass_back_d(0)

        return 0

    lax.fori_loop(0, steps, functools.partial(backward, 0, A1), 0)

    def through_norm(t, _):
        da = ACC[rows(t)].astype(BF16).astype(F32)
        wide = H[rows(t)].astype(F32)
        scale = lax.rsqrt(jnp.mean(wide * wide, -1, keepdims=True) + 1e-6)
        along = jnp.mean(da * wide, -1, keepdims=True)
        dh = (da * scale - wide * (scale * scale * scale * along)).astype(BF16).astype(F32)
        DY[rows(t)] = (DY[rows(t)].astype(F32) + dh).astype(BF16)
        AT[:, rows(t)] = A0[rows(t)].T
        return 0

    lax.fori_loop(0, tiles, through_norm, 0)
    lax.fori_loop(0, steps, functools.partial(backward, 1, A0), 0)

    last = 2 * steps - 1
    pass_on_d(1, 3)
    pass_on(last - 1)
    pass_on_d(1, 2)
    pass_on(last)
    pass_back_d(1)
    pass_back(last - 2)
    pass_back(last - 1)
    pass_back(last)

    def finish(k, _):
        p, i = k // steps, k % steps
        l = 1 - p
        cols = pl.ds(pl.multiple_of(column(i) * CHUNK, CHUNK), CHUNK)

        def put(total):
            gg_ref[l, :, cols] = total[0].astype(BF16)
            gu_ref[l, :, cols] = total[1].astype(BF16)

        @pl.when(end)
        def _():
            to_end(k).wait_recv()
            put(fin[k] + RM[k, 0].astype(F32))

        @pl.when(mid)
        def _():
            from_end(k, 1).wait_recv()
            across(k, 2).wait_recv()
            put(fin[k] + RE[k, 0].astype(F32) + RM[k, 1].astype(F32))

        return 0

    def finish_d(p):
        @pl.when(end)
        def _():
            to_end_d(p).wait_recv()
            gd_ref[1 - p] = (find[p] + RMd[p, 0].astype(F32)).astype(BF16)

        @pl.when(mid)
        def _():
            from_end_d(p, 1).wait_recv()
            across_d(p, 2).wait_recv()
            gd_ref[1 - p] = (find[p] + REd[p, 0].astype(F32) + RMd[p, 1].astype(F32)).astype(BF16)

    finish_d(0)
    finish_d(1)
    lax.fori_loop(0, 2 * steps, finish, 0)

    def sent(k, _):
        @pl.when(end)
        def _():
            for q in (3, 2, 1):
                from_end(k, q).wait_send()

        @pl.when(mid)
        def _():
            across(k, 3).wait_send()
            across(k, 2).wait_send()
            to_end(k).wait_send()

        return 0

    lax.fori_loop(0, 2 * steps, sent, 0)
    for p in range(2):

        @pl.when(end)
        def _():
            for q in (3, 2, 1):
                from_end_d(p, q).wait_send()

        @pl.when(mid)
        def _():
            across_d(p, 3).wait_send()
            across_d(p, 2).wait_send()
            to_end_d(p).wait_send()


def gradients(x, dy, wg, wu, wd):
    T, D = x.shape
    L, _, FF = wg.shape
    n = L * (FF // CHUNK)
    RG, RD = D // 8, FF // 8
    V, DMA = pltpu.VMEM, pltpu.SemaphoreType.DMA
    piece = (2, RG, CHUNK)
    return pl.pallas_call(
        functools.partial(gradients_kernel, T, D, FF),
        out_shape=[
            jax.ShapeDtypeStruct((L, RG, FF), BF16),
            jax.ShapeDtypeStruct((L, RG, FF), BF16),
            jax.ShapeDtypeStruct((L, RD, D), BF16),
        ],
        in_specs=[pl.BlockSpec(memory_space=pl.ANY)] * 5,
        out_specs=[pl.BlockSpec(memory_space=pltpu.VMEM)] * 3,
        scratch_shapes=[
            V((T, D), BF16), V((T, D), BF16), V((T, D), BF16), V((D, T), BF16), V((T, D), BF16), V((T, D), F32),
            V((T, CHUNK), BF16), V((T, CHUNK), BF16), V((T, CHUNK), BF16),
            V((2, D, CHUNK), BF16), V((2, D, CHUNK), BF16), V((2, CHUNK, D), BF16),
            V((4, 4, 2, *piece), BF16), V((n, 4, *piece), BF16), V((n, *piece), F32),
            V((n, 3, *piece), BF16), V((n, 2, *piece), BF16),
            V((L, FF, D), BF16), V((L, 4, RD, D), BF16), V((L, RD, D), F32),
            V((L, 3, RD, D), BF16), V((L, 2, RD, D), BF16),
            DMA((2, 3)), DMA((2,)), DMA((n,)), DMA((n,)), DMA((n, 3)), DMA((n, 3)), DMA((n,)), DMA((n, 2)),
            DMA((L, 4)), DMA((L, 4)), DMA((L, 3)), DMA((L, 3)), DMA((L,)), DMA((L, 2)),
        ],
        compiler_params=pltpu.CompilerParams(collective_id=0, has_side_effects=True, vmem_limit_bytes=VMEM_LIMIT),
        name="gradients",
    )(x, dy, wg, wu, wd)


def update_kernel(count, *refs):
    g_hbm, m_hbm, v_hbm, w_hbm = refs[0:3], refs[3:6], refs[6:9], refs[9:12]
    w_out, m_out, v_out = refs[12:15], refs[15:18], refs[18:21]
    g_s, m_s, v_s, w_s, n_s = refs[21:24], refs[24:27], refs[27:30], refs[30:33], refs[33:36]
    sq, in_sem, sq_send, sq_recv, r_send, r_recv, l_send, l_recv, p_send, p_recv, own_sem, mv_sem = refs[36:]
    me, z, c, h, end = placed()
    partner = z * 2 + 1 - c
    L = 2
    parts = [(l, t) for l in (1, 0) for t in (2, 0, 1)]

    loads = []
    for t in range(3):
        block = pl.ds(pl.multiple_of(me * g_s[t].shape[1], 32), g_s[t].shape[1])
        loads.append([
            pltpu.make_async_copy(g_hbm[t], g_s[t], in_sem.at[t, 0]),
            pltpu.make_async_copy(m_hbm[t], m_s[t], in_sem.at[t, 1]),
            pltpu.make_async_copy(v_hbm[t], v_s[t], in_sem.at[t, 2]),
            pltpu.make_async_copy(w_hbm[t].at[:, block], w_s[t], in_sem.at[t, 3]),
        ])
    for which in range(4):
        for t in (2, 0, 1):
            loads[t][which].start()

    barrier = pltpu.get_barrier_semaphore()
    for other in range(1, 8):
        pl.semaphore_signal(barrier, inc=1, device_id={"dp": (me + other) % 8}, device_id_type=MESH)

    STEP = 16

    def strip(r):
        return pl.ds(pl.multiple_of(r * STEP, STEP), STEP)

    total = jnp.zeros((8, 128), F32)
    for t in range(3):
        loads[t][0].wait()
        R, C = g_s[t].shape[1:]

        def squares(r, total, t=t, R=R, C=C):
            l, q = r // (R // STEP), r % (R // STEP)
            g = g_s[t][l, strip(q)].astype(F32)
            return total + jnp.sum((g * g).reshape(STEP // 8, 8, C // 128, 128), axis=(0, 2))

        total = lax.fori_loop(0, L * (R // STEP), squares, total)
    sq[me] = total
    pl.semaphore_wait(barrier, 7)

    def tell(other):
        to = (me + other) % 8
        return remote(sq.at[me], sq.at[me], sq_send.at[other], sq_recv.at[8 - other], to)

    def told(other):
        src = (me + other) % 8
        return remote(sq.at[src], sq.at[src], sq_send.at[8 - other], sq_recv.at[other], me)

    for other in range(1, 8):
        tell(other).start()
    for t in range(3):
        for which in (1, 2, 3):
            loads[t][which].wait()
    for other in range(1, 8):
        told(other).wait_recv()
    for other in range(1, 8):
        tell(other).wait_send()
    whole = jnp.full((8, 128), jnp.sum(sq[...]), F32)
    factor = jnp.minimum(1.0, 0.5 * lax.rsqrt(whole / count + 1e-30))[0:1, 0:1]

    def block(p, zt, ct):
        l, t = parts[p]
        R = g_s[t].shape[1]
        return w_out[t].at[l, pl.ds(pl.multiple_of((2 * zt + ct) * R, 32), R)]

    def mine(p):
        l, t = parts[p]
        return n_s[t].at[l]

    def to_right(p, hop):
        src = mine(p) if hop == 0 else block(p, z - hop, c)
        return remote(src, block(p, z - hop, c), r_send.at[p, hop], r_recv.at[p, hop], (z + 1) * 2 + c)

    def to_left(p, hop):
        src = mine(p) if hop == 0 else block(p, z + hop, c)
        return remote(src, block(p, z + hop, c), l_send.at[p, hop], l_recv.at[p, hop], (z - 1) * 2 + c)

    def to_partner(p, zt, own=False):
        return remote(mine(p) if own else block(p, zt, c), block(p, zt, c), p_send.at[p, zt], p_recv.at[p, zt], partner)

    def keep(p):
        return pltpu.make_async_copy(mine(p), block(p, z, c), own_sem.at[p])

    def moments(p):
        l, t = parts[p]
        return (
            pltpu.make_async_copy(m_s[t].at[l], m_out[t].at[l], mv_sem.at[p, 0]),
            pltpu.make_async_copy(v_s[t].at[l], v_out[t].at[l], mv_sem.at[p, 1]),
        )

    for p, (l, t) in enumerate(parts):

        def adamw(r, _, l=l, t=t):
            at = strip(r)
            g = g_s[t][l, at].astype(F32) * factor
            w = w_s[t][l, at].astype(F32)
            m = 0.9 * m_s[t][l, at] + 0.1 * g
            v = 0.95 * v_s[t][l, at] + 0.05 * g * g
            m_s[t][l, at] = m
            v_s[t][l, at] = v
            n_s[t][l, at] = (w - 0.02 * (m * lax.rsqrt(v + 1e-8) + 0.1 * w)).astype(BF16)
            return 0

        lax.fori_loop(0, g_s[t].shape[1] // STEP, adamw, 0)

        @pl.when(z < 3)
        def _():
            to_right(p, 0).start()

        @pl.when(z > 0)
        def _():
            to_left(p, 0).start()

        to_partner(p, z, True).start()
        keep(p).start()
        for copy in moments(p):
            copy.start()

    n = len(parts)
    for hop in range(3):
        for p in range(n):

            @pl.when(z > hop)
            def _():
                to_right(p, hop).wait_recv()

                if hop < 2:

                    @pl.when(z < 3)
                    def _():
                        to_right(p, hop + 1).start()

                to_partner(p, z - hop - 1).start()

            @pl.when(z + hop < 3)
            def _():
                to_left(p, hop).wait_recv()

                if hop < 2:

                    @pl.when(z > 0)
                    def _():
                        to_left(p, hop + 1).start()

                to_partner(p, z + hop + 1).start()

    for p in range(n):
        for zt in range(4):
            to_partner(p, zt).wait_recv()
    for p in range(n):
        keep(p).wait()
        for copy in moments(p):
            copy.wait()
        for zt in range(4):
            to_partner(p, zt).wait_send()
        for hop in range(3):

            @pl.when(jnp.logical_and(z < 3, z >= hop))
            def _():
                to_right(p, hop).wait_send()

            @pl.when(jnp.logical_and(z > 0, z + hop <= 3))
            def _():
                to_left(p, hop).wait_send()


def update(g, m, v, w):
    V, DMA = pltpu.VMEM, pltpu.SemaphoreType.DMA
    S = jax.ShapeDtypeStruct
    count = 8 * sum(a.size for a in g)
    out = [S(a.shape, BF16) for a in w] + [S(a.shape, F32) for a in (*m, *v)]
    return pl.pallas_call(
        functools.partial(update_kernel, float(count)),
        out_shape=out,
        in_specs=[pl.BlockSpec(memory_space=pl.ANY)] * 12,
        out_specs=[pl.BlockSpec(memory_space=pl.ANY)] * 9,
        scratch_shapes=[
            *(V(a.shape, BF16) for a in g), *(V(a.shape, F32) for a in m), *(V(a.shape, F32) for a in v),
            *(V(a.shape, BF16) for a in g), *(V(a.shape, BF16) for a in g),
            V((8, 8, 128), F32), DMA((3, 4)), DMA((8,)), DMA((8,)),
            DMA((6, 3)), DMA((6, 3)), DMA((6, 3)), DMA((6, 3)), DMA((6, 4)), DMA((6, 4)), DMA((6,)), DMA((6, 2)),
        ],
        compiler_params=pltpu.CompilerParams(collective_id=1, has_side_effects=True, vmem_limit_bytes=VMEM_LIMIT),
        name="update",
    )(*g, *m, *v, *w)


def solution(mesh):
    def step(x, dy, *arrays):
        w, m, v = (arrays[i : i + 3] for i in (0, 3, 6))
        g = gradients(x[0], dy[0], *w)
        return tuple(update(g, m, v, w))

    whole, split = P(None, None, None), P(None, "dp", None)
    return jax.shard_map(
        step,
        mesh=mesh,
        in_specs=(P(("rep", "dp")),) * 2 + (whole,) * 3 + (split,) * 6,
        out_specs=(P("rep", None, None),) * 3 + (P("rep", "dp", None),) * 6,
        check_vma=False,
    )
```

```python
import functools

import jax
import jax.numpy as jnp
from jax import lax
from jax.experimental import pallas as pl
from jax.experimental.pallas import tpu as pltpu
from jax.sharding import PartitionSpec as P

F32, BF16 = jnp.float32, jnp.bfloat16
MESH = pl.DeviceIdType.MESH
VMEM_LIMIT = 67_043_328
CHUNK = 256


def dot(a, b, ca=1, cb=0):
    return lax.dot_general(a, b, (((ca,), (cb,)), ((), ())), preferred_element_type=F32)


def placed():
    me = lax.axis_index("dp")
    z, c = me // 2, me % 2
    h = z // 2
    end = (z + h) % 2 == 0
    return me, z, c, h, end


def remote(src, dst, send, recv, to):
    return pltpu.make_async_remote_copy(
        src_ref=src, dst_ref=dst, send_sem=send, recv_sem=recv, device_id={"dp": to}, device_id_type=MESH
    )


def gradients_kernel(
    T, D, FF, x_hbm, dy_hbm, wg_hbm, wu_hbm, wd_hbm, gg_ref, gu_ref, gd_ref,
    H, A0, A1, AT, DY, ACC, hid, dg, du, wgs, wus, wds,
    own, prec, fin, RE, RM, ownd, precd, find, REd, RMd,
    w_sem, in_sem, d_send, d_recv, e_send, e_recv, m_send, m_recv,
    dd_send, dd_recv, ed_send, ed_recv, md_send, md_recv,
):
    me, z, c, h, end = placed()
    partner = z * 2 + 1 - c
    d = 1 - 2 * h
    inward, outward = (z + d) * 2 + c, (z - d) * 2 + c
    mid = jnp.logical_not(end)
    TT = min(512, T)
    tiles = T // TT
    steps = FF // CHUNK
    RG, RD = D // 8, FF // 8

    def target(q):
        return q + h * (3 - 2 * q)

    def column(i):
        return (i + steps - 2) % steps

    def rows(t):
        return pl.ds(pl.multiple_of(t * TT, TT), TT)

    def weights(l, i, s):
        cols = pl.ds(pl.multiple_of(column(i) * CHUNK, CHUNK), CHUNK)
        slot = s % 2
        return (
            pltpu.make_async_copy(wg_hbm.at[l, :, cols], wgs.at[slot], w_sem.at[slot, 0]),
            pltpu.make_async_copy(wu_hbm.at[l, :, cols], wus.at[slot], w_sem.at[slot, 1]),
            pltpu.make_async_copy(wd_hbm.at[l, cols, :], wds.at[slot], w_sem.at[slot, 2]),
        )

    get_x = pltpu.make_async_copy(x_hbm, H, in_sem.at[0])
    get_dy = pltpu.make_async_copy(dy_hbm, DY, in_sem.at[1])
    get_x.start()
    for copy in weights(0, 0, 0):
        copy.start()
    get_dy.start()

    barrier = pltpu.get_barrier_semaphore()
    pl.semaphore_signal(barrier, inc=1, device_id={"dp": partner}, device_id_type=MESH)
    pl.semaphore_signal(barrier, inc=1, device_id={"dp": inward}, device_id_type=MESH)

    @pl.when(mid)
    def _():
        pl.semaphore_signal(barrier, inc=1, device_id={"dp": outward}, device_id_type=MESH)
        pl.semaphore_wait(barrier, 3)

    @pl.when(end)
    def _():
        pl.semaphore_wait(barrier, 2)

    def normed(wide):
        return wide * lax.rsqrt(jnp.mean(wide * wide, -1, keepdims=True) + 1e-6)

    get_x.wait()

    def first(t, _):
        A0[rows(t)] = normed(H[rows(t)].astype(F32)).astype(BF16)
        ACC[rows(t)] = jnp.zeros((TT, D), F32)
        return 0

    lax.fori_loop(0, tiles, first, 0)

    def next_weights(l, i, s, after):
        for copy in weights(l, i, s):
            copy.wait()

        @pl.when(i < steps - 1)
        def _():
            for copy in weights(l, i + 1, s + 1):
                copy.start()

        if after is not None:

            @pl.when(i == steps - 1)
            def _():
                for copy in weights(after, 0, s + 1):
                    copy.start()

    def forward(i, _):
        next_weights(0, i, i, 1)
        slot = i % 2

        def tile(t, _):
            a = A0[rows(t)]
            gate, up = dot(a, wgs[slot]), dot(a, wus[slot])
            hidden = (gate * lax.logistic(gate) * up).astype(BF16)
            down = dot(hidden, wds[slot])

            ACC[rows(t)] += down
            return 0

        lax.fori_loop(0, tiles, tile, 0)
        return 0

    lax.fori_loop(0, steps, forward, 0)

    def between(t, _):
        out = ACC[rows(t)].astype(BF16).astype(F32)
        ACC[rows(t)] = jnp.zeros((TT, D), F32)
        h1 = (H[rows(t)].astype(F32) + out).astype(BF16)
        H[rows(t)] = h1
        a = normed(h1.astype(F32)).astype(BF16)
        A1[rows(t)] = a
        AT[:, rows(t)] = a.T
        return 0

    lax.fori_loop(0, tiles, between, 0)
    get_dy.wait()

    def to_partner(k):
        return remote(own.at[k % 4, :, 1 - c], prec.at[k], d_send.at[k], d_recv.at[k], partner)

    def to_partner_d(p, zt):
        block = pl.ds(pl.multiple_of((2 * zt + 1 - c) * RD, RD), RD)
        return remote(ownd.at[p, block], precd.at[p, zt], dd_send.at[p, zt], dd_recv.at[p, zt], partner)

    def from_end(k, q):
        return remote(prec.at[k, target(q)], RE.at[k, q - 1], e_send.at[k, q - 1], e_recv.at[k, q - 1], inward)

    def across(k, q):
        return remote(prec.at[k, target(q)], RM.at[k, 3 - q], e_send.at[k, q - 1], m_recv.at[k, 3 - q], inward)

    def to_end(k):
        return remote(prec.at[k, target(0)], RM.at[k, 0], m_send.at[k], m_recv.at[k, 0], outward)

    def from_end_d(p, q):
        return remote(precd.at[p, target(q)], REd.at[p, q - 1], ed_send.at[p, q - 1], ed_recv.at[p, q - 1], inward)

    def across_d(p, q):
        return remote(precd.at[p, target(q)], RMd.at[p, 3 - q], ed_send.at[p, q - 1], md_recv.at[p, 3 - q], inward)

    def to_end_d(p):
        return remote(precd.at[p, target(0)], RMd.at[p, 0], md_send.at[p], md_recv.at[p, 0], outward)

    def both(k, zt):
        return own[k % 4, zt, c].astype(F32) + prec[k, zt].astype(F32)

    def both_d(p, zt):
        block = pl.ds(pl.multiple_of((2 * zt + c) * RD, RD), RD)
        return ownd[p, block].astype(F32) + precd[p, zt].astype(F32)

    def share(k):
        to_partner(k).wait()
        fin[k] = both(k, z)

        @pl.when(end)
        def _():
            for q in (3, 2, 1):
                prec[k, target(q)] = both(k, target(q)).astype(BF16)
                from_end(k, q).start()

    def share_d(p, zt):
        to_partner_d(p, zt).wait()
        q = zt + h * (3 - 2 * zt)

        @pl.when(zt == z)
        def _():
            find[p] = both_d(p, zt)

        @pl.when(jnp.logical_and(end, zt != z))
        def _():
            precd[p, zt] = both_d(p, zt).astype(BF16)
            from_end_d(p, q).start()

    def pass_on(k):
        @pl.when(mid)
        def _():
            for q in (3, 2):
                from_end(k, q).wait_recv()
                prec[k, target(q)] = (both(k, target(q)) + RE[k, q - 1].astype(F32)).astype(BF16)
                across(k, q).start()

    def pass_back(k):
        @pl.when(mid)
        def _():
            across(k, 3).wait_recv()
            prec[k, target(0)] = (both(k, target(0)) + RM[k, 0].astype(F32)).astype(BF16)
            to_end(k).start()

    def pass_on_d(p, q):
        @pl.when(mid)
        def _():
            from_end_d(p, q).wait_recv()
            precd[p, target(q)] = (both_d(p, target(q)) + REd[p, q - 1].astype(F32)).astype(BF16)
            across_d(p, q).start()

    def pass_back_d(p):
        @pl.when(mid)
        def _():
            across_d(p, 3).wait_recv()
            precd[p, target(0)] = (both_d(p, target(0)) + RMd[p, 0].astype(F32)).astype(BF16)
            to_end_d(p).start()

    def backward(p, A, i, _):
        l = 1 - p
        s = steps * (1 + p) + i
        k = steps * p + i
        slot = s % 2
        j = column(i)
        next_weights(l, i, s, 0 if p == 0 else None)

        def tile(t, _):
            a = A[rows(t)]
            gate, up = dot(a, wgs[slot]), dot(a, wus[slot])
            dh = dot(DY[rows(t)], wds[slot], 1, 1).astype(BF16).astype(F32)
            sig = lax.logistic(gate)
            act = gate * sig
            hid[rows(t)] = (act * up).astype(BF16)
            du[rows(t)] = (dh * act).astype(BF16)
            dg[rows(t)] = (dh * up * (sig * (1.0 + gate * (1.0 - sig)))).astype(BF16)
            return 0

        lax.fori_loop(0, tiles, tile, 0)
        here = pl.ds(pl.multiple_of(j * CHUNK, CHUNK), CHUNK)
        ownd[p, here] = dot(hid[...], DY[...], 0, 0).astype(BF16)
        zt = (i // 2 + 3) % 4
        down_ready = jnp.logical_or(i % 2 == 1, i == steps - 1)

        @pl.when(down_ready)
        def _():
            to_partner_d(p, zt).start()

        own[k % 4, :, :, 0] = dot(AT[...], dg[...]).astype(BF16).reshape(4, 2, RG, CHUNK)
        own[k % 4, :, :, 1] = dot(AT[...], du[...]).astype(BF16).reshape(4, 2, RG, CHUNK)
        to_partner(k).start()

        if p == 0:

            def back(t, _):
                da = dot(dg[rows(t)], wgs[slot], 1, 1) + dot(du[rows(t)], wus[slot], 1, 1)
                ACC[rows(t)] += da
                return 0

            lax.fori_loop(0, tiles, back, 0)

        @pl.when(down_ready)
        def _():
            share_d(p, zt)

        share(k)

        @pl.when(k >= 2)
        def _():
            pass_on(k - 2)

        @pl.when(k >= 3)
        def _():
            pass_back(k - 3)

        if p == 1:

            @pl.when(i == 3)
            def _():
                pass_on_d(0, 3)
                pass_on_d(0, 2)
                pass_back_d(0)

        return 0

    lax.fori_loop(0, steps, functools.partial(backward, 0, A1), 0)

    def through_norm(t, _):
        da = ACC[rows(t)].astype(BF16).astype(F32)
        wide = H[rows(t)].astype(F32)
        scale = lax.rsqrt(jnp.mean(wide * wide, -1, keepdims=True) + 1e-6)
        along = jnp.mean(da * wide, -1, keepdims=True)
        dh = (da * scale - wide * (scale * scale * scale * along)).astype(BF16).astype(F32)
        DY[rows(t)] = (DY[rows(t)].astype(F32) + dh).astype(BF16)
        AT[:, rows(t)] = A0[rows(t)].T
        return 0

    lax.fori_loop(0, tiles, through_norm, 0)
    lax.fori_loop(0, steps, functools.partial(backward, 1, A0), 0)

    last = 2 * steps - 1
    pass_on_d(1, 3)
    pass_on(last - 1)
    pass_on_d(1, 2)
    pass_on(last)
    pass_back_d(1)
    pass_back(last - 2)
    pass_back(last - 1)
    pass_back(last)

    def finish(k, _):
        p, i = k // steps, k % steps
        l = 1 - p
        cols = pl.ds(pl.multiple_of(column(i) * CHUNK, CHUNK), CHUNK)

        def put(total):
            gg_ref[l, :, cols] = total[0].astype(BF16)
            gu_ref[l, :, cols] = total[1].astype(BF16)

        @pl.when(end)
        def _():
            to_end(k).wait_recv()
            put(fin[k] + RM[k, 0].astype(F32))

        @pl.when(mid)
        def _():
            from_end(k, 1).wait_recv()
            across(k, 2).wait_recv()
            put(fin[k] + RE[k, 0].astype(F32) + RM[k, 1].astype(F32))

        return 0

    def finish_d(p):
        @pl.when(end)
        def _():
            to_end_d(p).wait_recv()
            gd_ref[1 - p] = (find[p] + RMd[p, 0].astype(F32)).astype(BF16)

        @pl.when(mid)
        def _():
            from_end_d(p, 1).wait_recv()
            across_d(p, 2).wait_recv()
            gd_ref[1 - p] = (find[p] + REd[p, 0].astype(F32) + RMd[p, 1].astype(F32)).astype(BF16)

    finish_d(0)
    finish_d(1)
    lax.fori_loop(0, 2 * steps, finish, 0)

    def sent(k, _):
        @pl.when(end)
        def _():
            for q in (3, 2, 1):
                from_end(k, q).wait_send()

        @pl.when(mid)
        def _():
            across(k, 3).wait_send()
            across(k, 2).wait_send()
            to_end(k).wait_send()

        return 0

    lax.fori_loop(0, 2 * steps, sent, 0)
    for p in range(2):

        @pl.when(end)
        def _():
            for q in (3, 2, 1):
                from_end_d(p, q).wait_send()

        @pl.when(mid)
        def _():
            across_d(p, 3).wait_send()
            across_d(p, 2).wait_send()
            to_end_d(p).wait_send()


def gradients(x, dy, wg, wu, wd):
    T, D = x.shape
    L, _, FF = wg.shape
    n = L * (FF // CHUNK)
    RG, RD = D // 8, FF // 8
    V, DMA = pltpu.VMEM, pltpu.SemaphoreType.DMA
    piece = (2, RG, CHUNK)
    return pl.pallas_call(
        functools.partial(gradients_kernel, T, D, FF),
        out_shape=[
            jax.ShapeDtypeStruct((L, RG, FF), BF16),
            jax.ShapeDtypeStruct((L, RG, FF), BF16),
            jax.ShapeDtypeStruct((L, RD, D), BF16),
        ],
        in_specs=[pl.BlockSpec(memory_space=pl.ANY)] * 5,
        out_specs=[pl.BlockSpec(memory_space=pltpu.VMEM)] * 3,
        scratch_shapes=[
            V((T, D), BF16), V((T, D), BF16), V((T, D), BF16), V((D, T), BF16), V((T, D), BF16), V((T, D), F32),
            V((T, CHUNK), BF16), V((T, CHUNK), BF16), V((T, CHUNK), BF16),
            V((2, D, CHUNK), BF16), V((2, D, CHUNK), BF16), V((2, CHUNK, D), BF16),
            V((4, 4, 2, *piece), BF16), V((n, 4, *piece), BF16), V((n, *piece), F32),
            V((n, 3, *piece), BF16), V((n, 2, *piece), BF16),
            V((L, FF, D), BF16), V((L, 4, RD, D), BF16), V((L, RD, D), F32),
            V((L, 3, RD, D), BF16), V((L, 2, RD, D), BF16),
            DMA((2, 3)), DMA((2,)), DMA((n,)), DMA((n,)), DMA((n, 3)), DMA((n, 3)), DMA((n,)), DMA((n, 2)),
            DMA((L, 4)), DMA((L, 4)), DMA((L, 3)), DMA((L, 3)), DMA((L,)), DMA((L, 2)),
        ],
        compiler_params=pltpu.CompilerParams(collective_id=0, has_side_effects=True, vmem_limit_bytes=VMEM_LIMIT),
        name="gradients",
    )(x, dy, wg, wu, wd)


def update_kernel(count, *refs):
    g_hbm, m_hbm, v_hbm, w_hbm = refs[0:3], refs[3:6], refs[6:9], refs[9:12]
    w_out, m_out, v_out = refs[12:15], refs[15:18], refs[18:21]
    g_s, m_s, v_s, w_s, n_s = refs[21:24], refs[24:27], refs[27:30], refs[30:33], refs[33:36]
    sq, in_sem, sq_send, sq_recv, r_send, r_recv, l_send, l_recv, p_send, p_recv, own_sem, mv_sem = refs[36:]
    me, z, c, h, end = placed()
    partner = z * 2 + 1 - c
    L = 2
    parts = [(l, t) for l in (1, 0) for t in (2, 0, 1)]

    loads = []
    for t in range(3):
        block = pl.ds(pl.multiple_of(me * g_s[t].shape[1], 32), g_s[t].shape[1])
        loads.append([
            pltpu.make_async_copy(g_hbm[t], g_s[t], in_sem.at[t, 0]),
            pltpu.make_async_copy(m_hbm[t], m_s[t], in_sem.at[t, 1]),
            pltpu.make_async_copy(v_hbm[t], v_s[t], in_sem.at[t, 2]),
            pltpu.make_async_copy(w_hbm[t].at[:, block], w_s[t], in_sem.at[t, 3]),
        ])
    for which in range(4):
        for t in (2, 0, 1):
            loads[t][which].start()

    barrier = pltpu.get_barrier_semaphore()
    for other in range(1, 8):
        pl.semaphore_signal(barrier, inc=1, device_id={"dp": (me + other) % 8}, device_id_type=MESH)

    STEP = 16

    def strip(r):
        return pl.ds(pl.multiple_of(r * STEP, STEP), STEP)

    total = jnp.zeros((8, 128), F32)
    for t in range(3):
        loads[t][0].wait()
        R, C = g_s[t].shape[1:]

        def squares(r, total, t=t, R=R, C=C):
            l, q = r // (R // STEP), r % (R // STEP)
            g = g_s[t][l, strip(q)].astype(F32)
            return total + jnp.sum((g * g).reshape(STEP // 8, 8, C // 128, 128), axis=(0, 2))

        total = lax.fori_loop(0, L * (R // STEP), squares, total)
    sq[me] = total
    pl.semaphore_wait(barrier, 7)

    def tell(other):
        to = (me + other) % 8
        return remote(sq.at[me], sq.at[me], sq_send.at[other], sq_recv.at[8 - other], to)

    def told(other):
        src = (me + other) % 8
        return remote(sq.at[src], sq.at[src], sq_send.at[8 - other], sq_recv.at[other], me)

    for other in range(1, 8):
        tell(other).start()
    for t in range(3):
        for which in (1, 2, 3):
            loads[t][which].wait()
    for other in range(1, 8):
        told(other).wait_recv()
    for other in range(1, 8):
        tell(other).wait_send()
    whole = jnp.full((8, 128), jnp.sum(sq[...]), F32)
    factor = jnp.minimum(1.0, 0.5 * lax.rsqrt(whole / count + 1e-30))[0:1, 0:1]

    def block(p, zt, ct):
        l, t = parts[p]
        R = g_s[t].shape[1]
        return w_out[t].at[l, pl.ds(pl.multiple_of((2 * zt + ct) * R, 32), R)]

    def mine(p):
        l, t = parts[p]
        return n_s[t].at[l]

    def to_right(p, hop):
        src = mine(p) if hop == 0 else block(p, z - hop, c)
        return remote(src, block(p, z - hop, c), r_send.at[p, hop], r_recv.at[p, hop], (z + 1) * 2 + c)

    def to_left(p, hop):
        src = mine(p) if hop == 0 else block(p, z + hop, c)
        return remote(src, block(p, z + hop, c), l_send.at[p, hop], l_recv.at[p, hop], (z - 1) * 2 + c)

    def to_partner(p, zt, own=False):
        return remote(mine(p) if own else block(p, zt, c), block(p, zt, c), p_send.at[p, zt], p_recv.at[p, zt], partner)

    def keep(p):
        return pltpu.make_async_copy(mine(p), block(p, z, c), own_sem.at[p])

    def moments(p):
        l, t = parts[p]
        return (
            pltpu.make_async_copy(m_s[t].at[l], m_out[t].at[l], mv_sem.at[p, 0]),
            pltpu.make_async_copy(v_s[t].at[l], v_out[t].at[l], mv_sem.at[p, 1]),
        )

    for p, (l, t) in enumerate(parts):

        def adamw(r, _, l=l, t=t):
            at = strip(r)
            g = g_s[t][l, at].astype(F32) * factor
            w = w_s[t][l, at].astype(F32)
            m = 0.9 * m_s[t][l, at] + 0.1 * g
            v = 0.95 * v_s[t][l, at] + 0.05 * g * g
            m_s[t][l, at] = m
            v_s[t][l, at] = v
            n_s[t][l, at] = (w - 0.02 * (m * lax.rsqrt(v + 1e-8) + 0.1 * w)).astype(BF16)
            return 0

        lax.fori_loop(0, g_s[t].shape[1] // STEP, adamw, 0)

        @pl.when(z < 3)
        def _():
            to_right(p, 0).start()

        @pl.when(z > 0)
        def _():
            to_left(p, 0).start()

        to_partner(p, z, True).start()
        keep(p).start()
        for copy in moments(p):
            copy.start()

    n = len(parts)
    for hop in range(3):
        for p in range(n):

            @pl.when(z > hop)
            def _():
                to_right(p, hop).wait_recv()

                if hop < 2:

                    @pl.when(z < 3)
                    def _():
                        to_right(p, hop + 1).start()

                to_partner(p, z - hop - 1).start()

            @pl.when(z + hop < 3)
            def _():
                to_left(p, hop).wait_recv()

                if hop < 2:

                    @pl.when(z > 0)
                    def _():
                        to_left(p, hop + 1).start()

                to_partner(p, z + hop + 1).start()

    for p in range(n):
        for zt in range(4):
            to_partner(p, zt).wait_recv()
    for p in range(n):
        keep(p).wait()
        for copy in moments(p):
            copy.wait()
        for zt in range(4):
            to_partner(p, zt).wait_send()
        for hop in range(3):

            @pl.when(jnp.logical_and(z < 3, z >= hop))
            def _():
                to_right(p, hop).wait_send()

            @pl.when(jnp.logical_and(z > 0, z + hop <= 3))
            def _():
                to_left(p, hop).wait_send()


def update(g, m, v, w):
    V, DMA = pltpu.VMEM, pltpu.SemaphoreType.DMA
    S = jax.ShapeDtypeStruct
    count = 8 * sum(a.size for a in g)
    out = [S(a.shape, BF16) for a in w] + [S(a.shape, F32) for a in (*m, *v)]
    return pl.pallas_call(
        functools.partial(update_kernel, float(count)),
        out_shape=out,
        in_specs=[pl.BlockSpec(memory_space=pltpu.HBM)] * 12,
        out_specs=[pl.BlockSpec(memory_space=pl.ANY)] * 9,
        scratch_shapes=[
            *(V(a.shape, BF16) for a in g), *(V(a.shape, F32) for a in m), *(V(a.shape, F32) for a in v),
            *(V(a.shape, BF16) for a in g), *(V(a.shape, BF16) for a in g),
            V((8, 8, 128), F32), DMA((3, 4)), DMA((8,)), DMA((8,)),
            DMA((6, 3)), DMA((6, 3)), DMA((6, 3)), DMA((6, 3)), DMA((6, 4)), DMA((6, 4)), DMA((6,)), DMA((6, 2)),
        ],
        compiler_params=pltpu.CompilerParams(collective_id=1, has_side_effects=True, vmem_limit_bytes=18_000_000),
        name="update",
    )(*g, *m, *v, *w)


def store_kernel(*refs):
    n = len(refs) // 2
    src, dst, sem = refs[:n], refs[n : 2 * n], refs[2 * n]
    copies = [pltpu.make_async_copy(src[i].at[l], dst[i].at[l], sem.at[i, l]) for i in range(n) for l in range(2)]
    for copy in copies:
        copy.start()
    for copy in copies:
        copy.wait()


def store(arrays):
    n = len(arrays)
    return pl.pallas_call(
        store_kernel,
        out_shape=[jax.ShapeDtypeStruct(a.shape, a.dtype) for a in arrays],
        in_specs=[pl.BlockSpec(memory_space=pl.ANY)] * n,
        out_specs=[pl.BlockSpec(memory_space=pltpu.HBM)] * n,
        scratch_shapes=[pltpu.SemaphoreType.DMA((n, 2))],
        compiler_params=pltpu.CompilerParams(vmem_limit_bytes=1_000_000),
        name="store",
    )(*arrays)


def solution(mesh):
    def step(x, dy, *arrays):
        w, m, v = (arrays[i : i + 3] for i in (0, 3, 6))
        g = gradients(x[0], dy[0], *w)
        return tuple(store(update(g, m, v, w)))

    whole, split = P(None, None, None), P(None, "dp", None)
    return jax.shard_map(
        step,
        mesh=mesh,
        in_specs=(P(("rep", "dp")),) * 2 + (whole,) * 3 + (split,) * 6,
        out_specs=(P("rep", None, None),) * 3 + (P("rep", "dp", None),) * 6,
        check_vma=False,
    )
```

```python
import functools

import jax
import jax.numpy as jnp
from jax import lax
from jax.experimental import pallas as pl
from jax.experimental.pallas import tpu as pltpu
from jax.sharding import PartitionSpec as P

F32, BF16 = jnp.float32, jnp.bfloat16
MESH = pl.DeviceIdType.MESH
VMEM_LIMIT = 67_043_328
CHUNK = 256


def dot(a, b, ca=1, cb=0):
    return lax.dot_general(a, b, (((ca,), (cb,)), ((), ())), preferred_element_type=F32)


def placed():
    me = lax.axis_index("dp")
    z, c = me // 2, me % 2
    h = z // 2
    end = (z + h) % 2 == 0
    return me, z, c, h, end


def remote(src, dst, send, recv, to):
    return pltpu.make_async_remote_copy(
        src_ref=src, dst_ref=dst, send_sem=send, recv_sem=recv, device_id={"dp": to}, device_id_type=MESH
    )


def gradients_kernel(
    T, D, FF, x_hbm, dy_hbm, wg_hbm, wu_hbm, wd_hbm, *refs
):
    moments, (gg_ref, gu_ref, gd_ref), lent = refs[:6], refs[6:9], refs[9:18]
    (
    H, A0, A1, AT, DY, ACC, hid, dg, du, wgs, wus, wds,
    own, prec, fin, RE, RM, ownd, precd, find, REd, RMd,
    w_sem, in_sem, d_send, d_recv, e_send, e_recv, m_send, m_recv,
    dd_send, dd_recv, ed_send, ed_recv, md_send, md_recv, lend_send, lend_recv,
    ) = refs[18:]
    me, z, c, h, end = placed()
    partner = z * 2 + 1 - c
    d = 1 - 2 * h
    inward, outward = (z + d) * 2 + c, (z - d) * 2 + c
    mid = jnp.logical_not(end)
    TT = min(512, T)
    tiles = T // TT
    steps = FF // CHUNK
    RG, RD = D // 8, FF // 8

    def target(q):
        return q + h * (3 - 2 * q)

    def column(i):
        return (i + steps - 2) % steps

    def rows(t):
        return pl.ds(pl.multiple_of(t * TT, TT), TT)

    def weights(l, i, s):
        cols = pl.ds(pl.multiple_of(column(i) * CHUNK, CHUNK), CHUNK)
        slot = s % 2
        return (
            pltpu.make_async_copy(wg_hbm.at[l, :, cols], wgs.at[slot], w_sem.at[slot, 0]),
            pltpu.make_async_copy(wu_hbm.at[l, :, cols], wus.at[slot], w_sem.at[slot, 1]),
            pltpu.make_async_copy(wd_hbm.at[l, cols, :], wds.at[slot], w_sem.at[slot, 2]),
        )

    get_x = pltpu.make_async_copy(x_hbm, H, in_sem.at[0])
    get_dy = pltpu.make_async_copy(dy_hbm, DY, in_sem.at[1])
    get_x.start()
    for copy in weights(0, 0, 0):
        copy.start()
    get_dy.start()

    barrier = pltpu.get_barrier_semaphore()
    pl.semaphore_signal(barrier, inc=1, device_id={"dp": partner}, device_id_type=MESH)
    pl.semaphore_signal(barrier, inc=1, device_id={"dp": inward}, device_id_type=MESH)

    @pl.when(mid)
    def _():
        pl.semaphore_signal(barrier, inc=1, device_id={"dp": outward}, device_id_type=MESH)

    def lend(n):
        src = moments[n].at[1] if n < 6 else (gg_ref, gu_ref, gd_ref)[n - 6].at[1]
        return remote(src, lent[n], lend_send.at[n], lend_recv.at[n], outward)

    def normed(wide):
        return wide * lax.rsqrt(jnp.mean(wide * wide, -1, keepdims=True) + 1e-6)

    get_x.wait()

    def first(t, _):
        A0[rows(t)] = normed(H[rows(t)].astype(F32)).astype(BF16)
        ACC[rows(t)] = jnp.zeros((TT, D), F32)
        return 0

    lax.fori_loop(0, tiles, first, 0)

    @pl.when(mid)
    def _():
        pl.semaphore_wait(barrier, 3)
        for n in range(6):
            lend(n).start()

    @pl.when(end)
    def _():
        pl.semaphore_wait(barrier, 2)


    def next_weights(l, i, s, after):
        for copy in weights(l, i, s):
            copy.wait()

        @pl.when(i < steps - 1)
        def _():
            for copy in weights(l, i + 1, s + 1):
                copy.start()

        if after is not None:

            @pl.when(i == steps - 1)
            def _():
                for copy in weights(after, 0, s + 1):
                    copy.start()

    def forward(i, _):
        next_weights(0, i, i, 1)
        slot = i % 2

        def tile(t, _):
            a = A0[rows(t)]
            gate, up = dot(a, wgs[slot]), dot(a, wus[slot])
            hidden = (gate * lax.logistic(gate) * up).astype(BF16)
            down = dot(hidden, wds[slot])

            ACC[rows(t)] += down
            return 0

        lax.fori_loop(0, tiles, tile, 0)
        return 0

    lax.fori_loop(0, steps, forward, 0)

    def between(t, _):
        out = ACC[rows(t)].astype(BF16).astype(F32)
        ACC[rows(t)] = jnp.zeros((TT, D), F32)
        h1 = (H[rows(t)].astype(F32) + out).astype(BF16)
        H[rows(t)] = h1
        a = normed(h1.astype(F32)).astype(BF16)
        A1[rows(t)] = a
        AT[:, rows(t)] = a.T
        return 0

    lax.fori_loop(0, tiles, between, 0)
    get_dy.wait()

    def to_partner(k):
        return remote(own.at[k % 4, :, 1 - c], prec.at[k], d_send.at[k], d_recv.at[k], partner)

    def to_partner_d(p, zt):
        block = pl.ds(pl.multiple_of((2 * zt + 1 - c) * RD, RD), RD)
        return remote(ownd.at[p, block], precd.at[p, zt], dd_send.at[p, zt], dd_recv.at[p, zt], partner)

    def from_end(k, q):
        return remote(prec.at[k, target(q)], RE.at[k, q - 1], e_send.at[k, q - 1], e_recv.at[k, q - 1], inward)

    def across(k, q):
        return remote(prec.at[k, target(q)], RM.at[k, 3 - q], e_send.at[k, q - 1], m_recv.at[k, 3 - q], inward)

    def to_end(k):
        return remote(prec.at[k, target(0)], RM.at[k, 0], m_send.at[k], m_recv.at[k, 0], outward)

    def from_end_d(p, q):
        return remote(precd.at[p, target(q)], REd.at[p, q - 1], ed_send.at[p, q - 1], ed_recv.at[p, q - 1], inward)

    def across_d(p, q):
        return remote(precd.at[p, target(q)], RMd.at[p, 3 - q], ed_send.at[p, q - 1], md_recv.at[p, 3 - q], inward)

    def to_end_d(p):
        return remote(precd.at[p, target(0)], RMd.at[p, 0], md_send.at[p], md_recv.at[p, 0], outward)

    def both(k, zt):
        return own[k % 4, zt, c].astype(F32) + prec[k, zt].astype(F32)

    def both_d(p, zt):
        block = pl.ds(pl.multiple_of((2 * zt + c) * RD, RD), RD)
        return ownd[p, block].astype(F32) + precd[p, zt].astype(F32)

    def share(k):
        to_partner(k).wait()
        fin[k] = both(k, z)

        @pl.when(end)
        def _():
            for q in (3, 2, 1):
                prec[k, target(q)] = both(k, target(q)).astype(BF16)
                from_end(k, q).start()

    def share_d(p, zt):
        to_partner_d(p, zt).wait()
        q = zt + h * (3 - 2 * zt)

        @pl.when(zt == z)
        def _():
            find[p] = both_d(p, zt)

        @pl.when(jnp.logical_and(end, zt != z))
        def _():
            precd[p, zt] = both_d(p, zt).astype(BF16)
            from_end_d(p, q).start()

    def pass_on(k):
        @pl.when(mid)
        def _():
            for q in (3, 2):
                from_end(k, q).wait_recv()
                prec[k, target(q)] = (both(k, target(q)) + RE[k, q - 1].astype(F32)).astype(BF16)
                across(k, q).start()

    def pass_back(k):
        @pl.when(mid)
        def _():
            across(k, 3).wait_recv()
            prec[k, target(0)] = (both(k, target(0)) + RM[k, 0].astype(F32)).astype(BF16)
            to_end(k).start()

    def pass_on_d(p, q):
        @pl.when(mid)
        def _():
            from_end_d(p, q).wait_recv()
            precd[p, target(q)] = (both_d(p, target(q)) + REd[p, q - 1].astype(F32)).astype(BF16)
            across_d(p, q).start()

    def pass_back_d(p):
        @pl.when(mid)
        def _():
            across_d(p, 3).wait_recv()
            precd[p, target(0)] = (both_d(p, target(0)) + RMd[p, 0].astype(F32)).astype(BF16)
            to_end_d(p).start()

    def finish(k, _):
        p, i = k // steps, k % steps
        l = 1 - p
        cols = pl.ds(pl.multiple_of(column(i) * CHUNK, CHUNK), CHUNK)

        def put(total):
            gg_ref[l, :, cols] = total[0].astype(BF16)
            gu_ref[l, :, cols] = total[1].astype(BF16)

        @pl.when(end)
        def _():
            to_end(k).wait_recv()
            put(fin[k] + RM[k, 0].astype(F32))

        @pl.when(mid)
        def _():
            from_end(k, 1).wait_recv()
            across(k, 2).wait_recv()
            put(fin[k] + RE[k, 0].astype(F32) + RM[k, 1].astype(F32))

        return 0

    def finish_d(p):
        @pl.when(end)
        def _():
            to_end_d(p).wait_recv()
            gd_ref[1 - p] = (find[p] + RMd[p, 0].astype(F32)).astype(BF16)

        @pl.when(mid)
        def _():
            from_end_d(p, 1).wait_recv()
            across_d(p, 2).wait_recv()
            gd_ref[1 - p] = (find[p] + REd[p, 0].astype(F32) + RMd[p, 1].astype(F32)).astype(BF16)

    def backward(p, A, i, _):
        l = 1 - p
        s = steps * (1 + p) + i
        k = steps * p + i
        slot = s % 2
        j = column(i)
        next_weights(l, i, s, 0 if p == 0 else None)

        def tile(t, _):
            a = A[rows(t)]
            gate, up = dot(a, wgs[slot]), dot(a, wus[slot])
            dh = dot(DY[rows(t)], wds[slot], 1, 1).astype(BF16).astype(F32)
            sig = lax.logistic(gate)
            act = gate * sig
            hid[rows(t)] = (act * up).astype(BF16)
            du[rows(t)] = (dh * act).astype(BF16)
            dg[rows(t)] = (dh * up * (sig * (1.0 + gate * (1.0 - sig)))).astype(BF16)
            return 0

        lax.fori_loop(0, tiles, tile, 0)
        here = pl.ds(pl.multiple_of(j * CHUNK, CHUNK), CHUNK)
        ownd[p, here] = dot(hid[...], DY[...], 0, 0).astype(BF16)
        zt = (i // 2 + 3) % 4
        down_ready = jnp.logical_or(i % 2 == 1, i == steps - 1)

        @pl.when(down_ready)
        def _():
            to_partner_d(p, zt).start()

        own[k % 4, :, :, 0] = dot(AT[...], dg[...]).astype(BF16).reshape(4, 2, RG, CHUNK)
        own[k % 4, :, :, 1] = dot(AT[...], du[...]).astype(BF16).reshape(4, 2, RG, CHUNK)
        to_partner(k).start()

        if p == 0:

            def back(t, _):
                da = dot(dg[rows(t)], wgs[slot], 1, 1) + dot(du[rows(t)], wus[slot], 1, 1)
                ACC[rows(t)] += da
                return 0

            lax.fori_loop(0, tiles, back, 0)

        @pl.when(down_ready)
        def _():
            share_d(p, zt)

        share(k)

        @pl.when(k >= 2)
        def _():
            pass_on(k - 2)

        @pl.when(k >= 3)
        def _():
            pass_back(k - 3)

        if p == 1:

            @pl.when(i == 3)
            def _():
                pass_on_d(0, 3)
                pass_on_d(0, 2)
                pass_back_d(0)

            @pl.when(jnp.logical_and(mid, i == 5))
            def _():
                finish_d(0)
                lax.fori_loop(0, steps, finish, 0)
                for n in range(6, 9):
                    lend(n).start()

        return 0

    lax.fori_loop(0, steps, functools.partial(backward, 0, A1), 0)

    def through_norm(t, _):
        da = ACC[rows(t)].astype(BF16).astype(F32)
        wide = H[rows(t)].astype(F32)
        scale = lax.rsqrt(jnp.mean(wide * wide, -1, keepdims=True) + 1e-6)
        along = jnp.mean(da * wide, -1, keepdims=True)
        dh = (da * scale - wide * (scale * scale * scale * along)).astype(BF16).astype(F32)
        DY[rows(t)] = (DY[rows(t)].astype(F32) + dh).astype(BF16)
        AT[:, rows(t)] = A0[rows(t)].T
        return 0

    lax.fori_loop(0, tiles, through_norm, 0)
    lax.fori_loop(0, steps, functools.partial(backward, 1, A0), 0)

    last = 2 * steps - 1
    pass_on_d(1, 3)
    pass_on(last - 1)
    pass_on_d(1, 2)
    pass_on(last)
    pass_back_d(1)
    pass_back(last - 2)
    pass_back(last - 1)
    pass_back(last)

    @pl.when(end)
    def _():
        finish_d(0)
        lax.fori_loop(0, steps, finish, 0)

    finish_d(1)
    lax.fori_loop(steps, 2 * steps, finish, 0)

    for n in range(9):

        @pl.when(end)
        def _():
            lend(n).wait_recv()

        @pl.when(mid)
        def _():
            lend(n).wait_send()


    def sent(k, _):
        @pl.when(end)
        def _():
            for q in (3, 2, 1):
                from_end(k, q).wait_send()

        @pl.when(mid)
        def _():
            across(k, 3).wait_send()
            across(k, 2).wait_send()
            to_end(k).wait_send()

        return 0

    lax.fori_loop(0, 2 * steps, sent, 0)
    for p in range(2):

        @pl.when(end)
        def _():
            for q in (3, 2, 1):
                from_end_d(p, q).wait_send()

        @pl.when(mid)
        def _():
            across_d(p, 3).wait_send()
            across_d(p, 2).wait_send()
            to_end_d(p).wait_send()


def gradients(x, dy, wg, wu, wd, moments):
    T, D = x.shape
    L, _, FF = wg.shape
    n = L * (FF // CHUNK)
    RG, RD = D // 8, FF // 8
    V, DMA = pltpu.VMEM, pltpu.SemaphoreType.DMA
    piece = (2, RG, CHUNK)
    return pl.pallas_call(
        functools.partial(gradients_kernel, T, D, FF),
        out_shape=[
            jax.ShapeDtypeStruct((L, RG, FF), BF16),
            jax.ShapeDtypeStruct((L, RG, FF), BF16),
            jax.ShapeDtypeStruct((L, RD, D), BF16),
            *(pltpu.HBM(a.shape[1:], F32) for a in moments),
            *(pltpu.HBM(a.shape[1:], BF16) for a in moments[:3]),
        ],
        in_specs=[pl.BlockSpec(memory_space=pl.ANY)] * 11,
        out_specs=[pl.BlockSpec(memory_space=pltpu.VMEM)] * 3 + [pl.BlockSpec(memory_space=pltpu.HBM)] * 9,
        scratch_shapes=[
            V((T, D), BF16), V((T, D), BF16), V((T, D), BF16), V((D, T), BF16), V((T, D), BF16), V((T, D), F32),
            V((T, CHUNK), BF16), V((T, CHUNK), BF16), V((T, CHUNK), BF16),
            V((2, D, CHUNK), BF16), V((2, D, CHUNK), BF16), V((2, CHUNK, D), BF16),
            V((4, 4, 2, *piece), BF16), V((n, 4, *piece), BF16), V((n, *piece), F32),
            V((n, 3, *piece), BF16), V((n, 2, *piece), BF16),
            V((L, FF, D), BF16), V((L, 4, RD, D), BF16), V((L, RD, D), F32),
            V((L, 3, RD, D), BF16), V((L, 2, RD, D), BF16),
            DMA((2, 3)), DMA((2,)), DMA((n,)), DMA((n,)), DMA((n, 3)), DMA((n, 3)), DMA((n,)), DMA((n, 2)),
            DMA((L, 4)), DMA((L, 4)), DMA((L, 3)), DMA((L, 3)), DMA((L,)), DMA((L, 2)), DMA((9,)), DMA((9,)),
        ],
        compiler_params=pltpu.CompilerParams(collective_id=0, has_side_effects=True, vmem_limit_bytes=VMEM_LIMIT),
        name="gradients",
    )(x, dy, wg, wu, wd, *moments)


def update_kernel(count, *refs):
    g_hbm, m_hbm, v_hbm, w_hbm, lent = refs[0:3], refs[3:6], refs[6:9], refs[9:12], refs[12:21]
    w_out, m_out, v_out, refs = refs[21:24], refs[24:27], refs[27:30], refs[30:]
    g_s, m_s, v_s, w_s, n_s = refs[0:3], refs[3:6], refs[6:9], refs[9:12], refs[12:15]
    g_n, m_n, v_n, w_n, n_n, refs = refs[15:18], refs[18:21], refs[21:24], refs[24:27], refs[27:30], refs[30:]
    sq, in_sem, sq_send, sq_recv, r_send, r_recv, l_send, l_recv, p_send, p_recv, own_sem, mv_sem, near_sem = refs
    me, z, c, h, end = placed()
    partner = z * 2 + 1 - c
    L = 2
    parts = [(l, t) for l in (0, 1) for t in (2, 0, 1)]
    inward = z + 1 - 2 * h

    loads = []
    for t in range(3):
        block = pl.ds(pl.multiple_of(me * g_s[t].shape[1], 32), g_s[t].shape[1])
        loads.append([
            pltpu.make_async_copy(g_hbm[t], g_s[t], in_sem.at[t, 0]),
            pltpu.make_async_copy(m_hbm[t], m_s[t], in_sem.at[t, 1]),
            pltpu.make_async_copy(v_hbm[t], v_s[t], in_sem.at[t, 2]),
            pltpu.make_async_copy(w_hbm[t].at[:, block], w_s[t], in_sem.at[t, 3]),
        ])
    for which in range(4):
        for t in (2, 0, 1):
            loads[t][which].start()

    near = []
    for t in range(3):
        block = pl.ds(pl.multiple_of((2 * inward + c) * g_s[t].shape[1], 32), g_s[t].shape[1])
        near += [
            pltpu.make_async_copy(lent[t], m_n[t], near_sem.at[t, 0]),
            pltpu.make_async_copy(lent[3 + t], v_n[t], near_sem.at[t, 1]),
            pltpu.make_async_copy(lent[6 + t], g_n[t], near_sem.at[t, 2]),
            pltpu.make_async_copy(w_hbm[t].at[1, block], w_n[t], near_sem.at[t, 3]),
        ]

    @pl.when(end)
    def _():
        for copy in near:
            copy.start()

    barrier = pltpu.get_barrier_semaphore()
    for other in range(1, 8):
        pl.semaphore_signal(barrier, inc=1, device_id={"dp": (me + other) % 8}, device_id_type=MESH)

    STEP = 16

    def strip(r):
        return pl.ds(pl.multiple_of(r * STEP, STEP), STEP)

    total = jnp.zeros((8, 128), F32)
    for t in range(3):
        loads[t][0].wait()
        R, C = g_s[t].shape[1:]

        def squares(r, total, t=t, R=R, C=C):
            l, q = r // (R // STEP), r % (R // STEP)
            g = g_s[t][l, strip(q)].astype(F32)
            return total + jnp.sum((g * g).reshape(STEP // 8, 8, C // 128, 128), axis=(0, 2))

        total = lax.fori_loop(0, L * (R // STEP), squares, total)
    sq[me] = total
    pl.semaphore_wait(barrier, 7)

    def tell(other):
        to = (me + other) % 8
        return remote(sq.at[me], sq.at[me], sq_send.at[other], sq_recv.at[8 - other], to)

    def told(other):
        src = (me + other) % 8
        return remote(sq.at[src], sq.at[src], sq_send.at[8 - other], sq_recv.at[other], me)

    for other in range(1, 8):
        tell(other).start()
    for t in range(3):
        for which in (1, 2, 3):
            loads[t][which].wait()
    for other in range(1, 8):
        told(other).wait_recv()
    for other in range(1, 8):
        tell(other).wait_send()
    whole = jnp.full((8, 128), jnp.sum(sq[...]), F32)
    factor = jnp.minimum(1.0, 0.5 * lax.rsqrt(whole / count + 1e-30))[0:1, 0:1]

    def block(p, zt, ct):
        l, t = parts[p]
        R = g_s[t].shape[1]
        return w_out[t].at[l, pl.ds(pl.multiple_of((2 * zt + ct) * R, 32), R)]

    def mine(p):
        l, t = parts[p]
        return n_s[t].at[l]

    def to_right(p, hop):
        src = mine(p) if hop == 0 else block(p, z - hop, c)
        return remote(src, block(p, z - hop, c), r_send.at[p, hop], r_recv.at[p, hop], (z + 1) * 2 + c)

    def to_left(p, hop):
        src = mine(p) if hop == 0 else block(p, z + hop, c)
        return remote(src, block(p, z + hop, c), l_send.at[p, hop], l_recv.at[p, hop], (z - 1) * 2 + c)

    def to_partner(p, zt, own=False):
        return remote(mine(p) if own else block(p, zt, c), block(p, zt, c), p_send.at[p, zt], p_recv.at[p, zt], partner)

    def keep(p):
        return pltpu.make_async_copy(mine(p), block(p, z, c), own_sem.at[p])

    def moments(p):
        l, t = parts[p]
        return (
            pltpu.make_async_copy(m_s[t].at[l], m_out[t].at[l], mv_sem.at[p, 0]),
            pltpu.make_async_copy(v_s[t].at[l], v_out[t].at[l], mv_sem.at[p, 1]),
        )

    def adamw(g, m, v, w):
        g, w = g.astype(F32) * factor, w.astype(F32)
        m = 0.9 * m + 0.1 * g
        v = 0.95 * v + 0.05 * g * g
        return (w - 0.02 * (m * lax.rsqrt(v + 1e-8) + 0.1 * w)).astype(BF16), m, v

    def sends_right(p, hop):
        if hop == 0 and parts[p][0] == 1:
            return jnp.logical_and(z < 3, z != 2)
        return jnp.logical_and(z < 3, z >= hop)

    def sends_left(p, hop):
        if hop == 0 and parts[p][0] == 1:
            return jnp.logical_and(z > 0, z != 1)
        return jnp.logical_and(z > 0, z + hop <= 3)

    for p, (l, t) in enumerate(parts):

        def own(r, _, l=l, t=t):
            at = strip(r)
            new, m, v = adamw(g_s[t][l, at], m_s[t][l, at], v_s[t][l, at], w_s[t][l, at])
            m_s[t][l, at] = m
            v_s[t][l, at] = v
            n_s[t][l, at] = new
            return 0

        lax.fori_loop(0, g_s[t].shape[1] // STEP, own, 0)

        @pl.when(sends_right(p, 0))
        def _():
            to_right(p, 0).start()

        @pl.when(sends_left(p, 0))
        def _():
            to_left(p, 0).start()

        to_partner(p, z, True).start()
        keep(p).start()
        for copy in moments(p):
            copy.start()

    def near_block(p):
        return block(p, inward, c)

    def near_keep(p):
        return pltpu.make_async_copy(n_n[parts[p][1]], near_block(p), own_sem.at[p])

    def near_to_partner(p):
        return remote(n_n[parts[p][1]], near_block(p), p_send.at[p, inward], p_recv.at[p, inward], partner)

    @pl.when(end)
    def _():
        for copy in near:
            copy.wait()
        for p, (l, t) in enumerate(parts):
            if l == 1:

                def neighbour(r, _, t=t):
                    at = strip(r)
                    n_n[t][at] = adamw(g_n[t][at], m_n[t][at], v_n[t][at], w_n[t][at])[0]
                    return 0

                lax.fori_loop(0, g_s[t].shape[1] // STEP, neighbour, 0)
                near_to_partner(p).start()
                keep(p).wait()
                near_keep(p).start()

    n = len(parts)
    for hop in range(3):
        for p in range(n):
            borrowed = hop == 0 and parts[p][0] == 1

            @pl.when(jnp.logical_and(z > hop, z != 3) if borrowed else z > hop)
            def _():
                to_right(p, hop).wait_recv()

                if hop < 2:

                    @pl.when(z < 3)
                    def _():
                        to_right(p, hop + 1).start()

                to_partner(p, z - hop - 1).start()

            @pl.when(jnp.logical_and(z + hop < 3, z != 0) if borrowed else z + hop < 3)
            def _():
                to_left(p, hop).wait_recv()

                if hop < 2:

                    @pl.when(z > 0)
                    def _():
                        to_left(p, hop + 1).start()

                to_partner(p, z + hop + 1).start()

    for p in range(n):
        for zt in range(4):
            to_partner(p, zt).wait_recv()
    for p in range(n):
        keep(p).wait()
        for copy in moments(p):
            copy.wait()
        for zt in range(4):
            to_partner(p, zt).wait_send()
        for hop in range(3):

            @pl.when(sends_right(p, hop))
            def _():
                to_right(p, hop).wait_send()

            @pl.when(sends_left(p, hop))
            def _():
                to_left(p, hop).wait_send()


def update(g, m, v, w, lent):
    V, DMA = pltpu.VMEM, pltpu.SemaphoreType.DMA
    S = jax.ShapeDtypeStruct
    count = 8 * sum(a.size for a in g)
    out = [V(a.shape, BF16) for a in w] + [V(a.shape, F32) for a in (*m, *v)]
    return pl.pallas_call(
        functools.partial(update_kernel, float(count)),
        out_shape=out,
        in_specs=[pl.BlockSpec(memory_space=pltpu.HBM)] * 21,
        out_specs=[pl.BlockSpec(memory_space=pl.ANY)] * 9,
        scratch_shapes=[
            *(V(a.shape, BF16) for a in g), *(V(a.shape, F32) for a in m), *(V(a.shape, F32) for a in v),
            *(V(a.shape, BF16) for a in g), *(V(a.shape, BF16) for a in g),
            *(V(a.shape[1:], BF16) for a in g), *(V(a.shape[1:], F32) for a in m), *(V(a.shape[1:], F32) for a in v),
            *(V(a.shape[1:], BF16) for a in g), *(V(a.shape[1:], BF16) for a in g),
            V((8, 8, 128), F32), DMA((3, 4)), DMA((8,)), DMA((8,)),
            DMA((6, 3)), DMA((6, 3)), DMA((6, 3)), DMA((6, 3)), DMA((6, 4)), DMA((6, 4)), DMA((6,)), DMA((6, 2)), DMA((3, 4)),
        ],
        compiler_params=pltpu.CompilerParams(collective_id=1, has_side_effects=True, vmem_limit_bytes=36_000_000),
        name="update",
    )(*g, *m, *v, *w, *lent)


def store_kernel(*refs):
    n = len(refs) // 2
    src, dst, sem = refs[:n], refs[n : 2 * n], refs[2 * n]
    copies = [pltpu.make_async_copy(src[i].at[l], dst[i].at[l], sem.at[i, l]) for i in range(n) for l in range(2)]
    for copy in copies:
        copy.start()
    for copy in copies:
        copy.wait()


def store(arrays):
    n = len(arrays)
    return pl.pallas_call(
        store_kernel,
        out_shape=[jax.ShapeDtypeStruct(a.shape, a.dtype) for a in arrays],
        in_specs=[pl.BlockSpec(memory_space=pl.ANY)] * n,
        out_specs=[pl.BlockSpec(memory_space=pltpu.HBM)] * n,
        scratch_shapes=[pltpu.SemaphoreType.DMA((n, 2))],
        compiler_params=pltpu.CompilerParams(vmem_limit_bytes=1_000_000),
        name="store",
    )(*arrays)


def solution(mesh):
    def step(x, dy, *arrays):
        w, m, v = (arrays[i : i + 3] for i in (0, 3, 6))
        out = gradients(x[0], dy[0], *w, (*m, *v))
        return tuple(store(update(out[:3], m, v, w, out[3:])))

    whole, split = P(None, None, None), P(None, "dp", None)
    return jax.shard_map(
        step,
        mesh=mesh,
        in_specs=(P(("rep", "dp")),) * 2 + (whole,) * 3 + (split,) * 6,
        out_specs=(P("rep", None, None),) * 3 + (P("rep", "dp", None),) * 6,
        check_vma=False,
    )
```

```python
import functools

import jax
import jax.numpy as jnp
from jax import lax
from jax.experimental import pallas as pl
from jax.experimental.pallas import tpu as pltpu
from jax.sharding import PartitionSpec as P

F32, BF16 = jnp.float32, jnp.bfloat16
MESH = pl.DeviceIdType.MESH
VMEM_LIMIT = 67_043_328
CHUNK = 256


def dot(a, b, ca=1, cb=0):
    return lax.dot_general(a, b, (((ca,), (cb,)), ((), ())), preferred_element_type=F32)


def placed():
    me = lax.axis_index("dp")
    z, c = me // 2, me % 2
    h = z // 2
    end = (z + h) % 2 == 0
    return me, z, c, h, end


def remote(src, dst, send, recv, to):
    return pltpu.make_async_remote_copy(
        src_ref=src, dst_ref=dst, send_sem=send, recv_sem=recv, device_id={"dp": to}, device_id_type=MESH
    )


def gradients_kernel(
    T, D, FF, x_hbm, dy_hbm, wg_hbm, wu_hbm, wd_hbm, *refs
):
    moments, (gg_ref, gu_ref, gd_ref), lent = refs[:6], refs[6:9], refs[9:18]
    (
    H, A0, A1, AT, DY, ACC, hid, dg, du, wgs, wus, wds,
    own, prec, fin, RE, RM, ownd, precd, find, REd, RMd,
    w_sem, in_sem, d_send, d_recv, e_send, e_recv, m_send, m_recv,
    dd_send, dd_recv, ed_send, ed_recv, md_send, md_recv, lend_send, lend_recv, x_sem,
    ) = refs[18:]
    me, z, c, h, end = placed()
    partner = z * 2 + 1 - c
    d = 1 - 2 * h
    inward, outward = (z + d) * 2 + c, (z - d) * 2 + c
    mid = jnp.logical_not(end)
    TT = min(512, T)
    tiles = T // TT
    steps = FF // CHUNK
    RG, RD = D // 8, FF // 8

    def target(q):
        return q + h * (3 - 2 * q)

    def column(i):
        return (i + steps - 2) % steps

    def rows(t):
        return pl.ds(pl.multiple_of(t * TT, TT), TT)

    def weights(l, i, s):
        cols = pl.ds(pl.multiple_of(column(i) * CHUNK, CHUNK), CHUNK)
        slot = s % 2
        return (
            pltpu.make_async_copy(wg_hbm.at[l, :, cols], wgs.at[slot], w_sem.at[slot, 0]),
            pltpu.make_async_copy(wu_hbm.at[l, :, cols], wus.at[slot], w_sem.at[slot, 1]),
            pltpu.make_async_copy(wd_hbm.at[l, cols, :], wds.at[slot], w_sem.at[slot, 2]),
        )

    def get_x(t):
        return pltpu.make_async_copy(x_hbm.at[rows(t)], H.at[rows(t)], x_sem.at[t])

    get_dy = pltpu.make_async_copy(dy_hbm, DY, in_sem.at[0])
    for t in range(tiles):
        get_x(t).start()
    for copy in weights(0, 0, 0):
        copy.start()
    get_dy.start()

    barrier = pltpu.get_barrier_semaphore()
    pl.semaphore_signal(barrier, inc=1, device_id={"dp": partner}, device_id_type=MESH)
    pl.semaphore_signal(barrier, inc=1, device_id={"dp": inward}, device_id_type=MESH)

    @pl.when(mid)
    def _():
        pl.semaphore_signal(barrier, inc=1, device_id={"dp": outward}, device_id_type=MESH)

    def lend(n):
        src = moments[n].at[1] if n < 6 else (gg_ref, gu_ref, gd_ref)[n - 6].at[1]
        return remote(src, lent[n], lend_send.at[n], lend_recv.at[n], outward)

    def normed(wide):
        return wide * lax.rsqrt(jnp.mean(wide * wide, -1, keepdims=True) + 1e-6)

    def first(t, _):
        get_x(t).wait()
        A0[rows(t)] = normed(H[rows(t)].astype(F32)).astype(BF16)
        ACC[rows(t)] = jnp.zeros((TT, D), F32)
        return 0

    lax.fori_loop(0, tiles, first, 0)

    @pl.when(mid)
    def _():
        pl.semaphore_wait(barrier, 3)
        for n in range(6):
            lend(n).start()

    @pl.when(end)
    def _():
        pl.semaphore_wait(barrier, 2)


    def next_weights(l, i, s, after):
        for copy in weights(l, i, s):
            copy.wait()

        @pl.when(i < steps - 1)
        def _():
            for copy in weights(l, i + 1, s + 1):
                copy.start()

        if after is not None:

            @pl.when(i == steps - 1)
            def _():
                for copy in weights(after, 0, s + 1):
                    copy.start()

    def forward(i, _):
        next_weights(0, i, i, 1)
        slot = i % 2

        def tile(t, _):
            a = A0[rows(t)]
            gate, up = dot(a, wgs[slot]), dot(a, wus[slot])
            hidden = (gate * lax.logistic(gate) * up).astype(BF16)
            down = dot(hidden, wds[slot])

            ACC[rows(t)] += down
            return 0

        lax.fori_loop(0, tiles, tile, 0)
        return 0

    lax.fori_loop(0, steps, forward, 0)

    def between(t, _):
        out = ACC[rows(t)].astype(BF16).astype(F32)
        ACC[rows(t)] = jnp.zeros((TT, D), F32)
        h1 = (H[rows(t)].astype(F32) + out).astype(BF16)
        H[rows(t)] = h1
        a = normed(h1.astype(F32)).astype(BF16)
        A1[rows(t)] = a
        AT[:, rows(t)] = a.T
        return 0

    lax.fori_loop(0, tiles, between, 0)
    get_dy.wait()

    def to_partner(k):
        return remote(own.at[k % 4, :, 1 - c], prec.at[k], d_send.at[k], d_recv.at[k], partner)

    def to_partner_d(p, zt):
        block = pl.ds(pl.multiple_of((2 * zt + 1 - c) * RD, RD), RD)
        return remote(ownd.at[p, block], precd.at[p, zt], dd_send.at[p, zt], dd_recv.at[p, zt], partner)

    def from_end(k, q):
        return remote(prec.at[k, target(q)], RE.at[k, q - 1], e_send.at[k, q - 1], e_recv.at[k, q - 1], inward)

    def across(k, q):
        return remote(prec.at[k, target(q)], RM.at[k, 3 - q], e_send.at[k, q - 1], m_recv.at[k, 3 - q], inward)

    def to_end(k):
        return remote(prec.at[k, target(0)], RM.at[k, 0], m_send.at[k], m_recv.at[k, 0], outward)

    def half(u):
        return pl.ds(u * (RD // 2), RD // 2)

    def from_end_d(p, q, u):
        src, dst = precd.at[p, target(q), half(u)], REd.at[p, q - 1, half(u)]
        return remote(src, dst, ed_send.at[p, q - 1, u], ed_recv.at[p, q - 1, u], inward)

    def across_d(p, q, u):
        src, dst = precd.at[p, target(q), half(u)], RMd.at[p, 3 - q, half(u)]
        return remote(src, dst, ed_send.at[p, q - 1, u], md_recv.at[p, 3 - q, u], inward)

    def to_end_d(p, u):
        src, dst = precd.at[p, target(0), half(u)], RMd.at[p, 0, half(u)]
        return remote(src, dst, md_send.at[p, u], md_recv.at[p, 0, u], outward)

    def both(k, zt):
        return own[k % 4, zt, c].astype(F32) + prec[k, zt].astype(F32)

    def both_d(p, zt, u):
        block = pl.ds(pl.multiple_of((2 * zt + c) * RD + u * (RD // 2), RD // 2), RD // 2)
        return ownd[p, block].astype(F32) + precd[p, zt, half(u)].astype(F32)

    def share(k):
        to_partner(k).wait()
        fin[k] = both(k, z)

        @pl.when(end)
        def _():
            for q in (3, 2, 1):
                prec[k, target(q)] = both(k, target(q)).astype(BF16)
                from_end(k, q).start()

    def share_d(p, zt):
        to_partner_d(p, zt).wait()
        q = zt + h * (3 - 2 * zt)

        @pl.when(zt == z)
        def _():
            for u in range(2):
                find[p, half(u)] = both_d(p, zt, u)

        @pl.when(jnp.logical_and(end, zt != z))
        def _():
            for u in range(2):
                precd[p, zt, half(u)] = both_d(p, zt, u).astype(BF16)
                from_end_d(p, q, u).start()

    def pass_on(k):
        @pl.when(mid)
        def _():
            for q in (3, 2):
                from_end(k, q).wait_recv()
                prec[k, target(q)] = (both(k, target(q)) + RE[k, q - 1].astype(F32)).astype(BF16)
                across(k, q).start()

    def pass_back(k):
        @pl.when(mid)
        def _():
            across(k, 3).wait_recv()
            prec[k, target(0)] = (both(k, target(0)) + RM[k, 0].astype(F32)).astype(BF16)
            to_end(k).start()

    def pass_on_d(p, q, u):
        @pl.when(mid)
        def _():
            from_end_d(p, q, u).wait_recv()
            total = both_d(p, target(q), u) + REd[p, q - 1, half(u)].astype(F32)
            precd[p, target(q), half(u)] = total.astype(BF16)
            across_d(p, q, u).start()

    def pass_back_d(p):
        @pl.when(mid)
        def _():
            for u in range(2):
                across_d(p, 3, u).wait_recv()
                total = both_d(p, target(0), u) + RMd[p, 0, half(u)].astype(F32)
                precd[p, target(0), half(u)] = total.astype(BF16)
                to_end_d(p, u).start()

    def finish(k, _):
        p, i = k // steps, k % steps
        l = 1 - p
        cols = pl.ds(pl.multiple_of(column(i) * CHUNK, CHUNK), CHUNK)

        def put(total):
            gg_ref[l, :, cols] = total[0].astype(BF16)
            gu_ref[l, :, cols] = total[1].astype(BF16)

        @pl.when(end)
        def _():
            to_end(k).wait_recv()
            put(fin[k] + RM[k, 0].astype(F32))

        @pl.when(mid)
        def _():
            from_end(k, 1).wait_recv()
            across(k, 2).wait_recv()
            put(fin[k] + RE[k, 0].astype(F32) + RM[k, 1].astype(F32))

        return 0

    def finish_d(p):
        @pl.when(end)
        def _():
            for u in range(2):
                to_end_d(p, u).wait_recv()
            gd_ref[1 - p] = (find[p] + RMd[p, 0].astype(F32)).astype(BF16)

        @pl.when(mid)
        def _():
            for u in range(2):
                from_end_d(p, 1, u).wait_recv()
                across_d(p, 2, u).wait_recv()
            gd_ref[1 - p] = (find[p] + REd[p, 0].astype(F32) + RMd[p, 1].astype(F32)).astype(BF16)

    def backward(p, A, i, _):
        l = 1 - p
        s = steps * (1 + p) + i
        k = steps * p + i
        slot = s % 2
        j = column(i)
        next_weights(l, i, s, 0 if p == 0 else None)

        def tile(t, _):
            a = A[rows(t)]
            gate, up = dot(a, wgs[slot]), dot(a, wus[slot])
            dh = dot(DY[rows(t)], wds[slot], 1, 1).astype(BF16).astype(F32)
            sig = lax.logistic(gate)
            act = gate * sig
            hid[rows(t)] = (act * up).astype(BF16)
            du[rows(t)] = (dh * act).astype(BF16)
            dg[rows(t)] = (dh * up * (sig * (1.0 + gate * (1.0 - sig)))).astype(BF16)
            return 0

        lax.fori_loop(0, tiles, tile, 0)
        here = pl.ds(pl.multiple_of(j * CHUNK, CHUNK), CHUNK)
        own[k % 4, :, :, 0] = dot(AT[...], dg[...]).astype(BF16).reshape(4, 2, RG, CHUNK)
        own[k % 4, :, :, 1] = dot(AT[...], du[...]).astype(BF16).reshape(4, 2, RG, CHUNK)
        to_partner(k).start()
        ownd[p, here] = dot(hid[...], DY[...], 0, 0).astype(BF16)
        zt = (i // 2 + 3) % 4
        down_ready = jnp.logical_or(i % 2 == 1, i == steps - 1)

        @pl.when(down_ready)
        def _():
            to_partner_d(p, zt).start()

        if p == 0:

            def back(t, _):
                da = dot(dg[rows(t)], wgs[slot], 1, 1) + dot(du[rows(t)], wus[slot], 1, 1)
                ACC[rows(t)] += da
                return 0

            lax.fori_loop(0, tiles, back, 0)

        @pl.when(down_ready)
        def _():
            share_d(p, zt)

        share(k)

        @pl.when(k >= 2)
        def _():
            pass_on(k - 2)

        @pl.when(k >= 3)
        def _():
            pass_back(k - 3)

        if p == 1:

            @pl.when(i == 2)
            def _():
                for q in (3, 2):
                    for u in range(2):
                        pass_on_d(0, q, u)
                pass_back_d(0)

            @pl.when(jnp.logical_and(mid, i == 3))
            def _():
                finish_d(0)
                lax.fori_loop(0, steps, finish, 0)
                for n in range(6, 9):
                    lend(n).start()

        return 0

    lax.fori_loop(0, steps, functools.partial(backward, 0, A1), 0)

    def through_norm(t, _):
        da = ACC[rows(t)].astype(BF16).astype(F32)
        wide = H[rows(t)].astype(F32)
        scale = lax.rsqrt(jnp.mean(wide * wide, -1, keepdims=True) + 1e-6)
        along = jnp.mean(da * wide, -1, keepdims=True)
        dh = (da * scale - wide * (scale * scale * scale * along)).astype(BF16).astype(F32)
        DY[rows(t)] = (DY[rows(t)].astype(F32) + dh).astype(BF16)
        AT[:, rows(t)] = A0[rows(t)].T
        return 0

    lax.fori_loop(0, tiles, through_norm, 0)
    lax.fori_loop(0, steps, functools.partial(backward, 1, A0), 0)

    last = 2 * steps - 1
    pass_on_d(1, 3, 0)
    pass_on_d(1, 3, 1)
    pass_on(last - 1)
    pass_on_d(1, 2, 0)
    pass_on(last)
    pass_on_d(1, 2, 1)
    pass_back_d(1)
    pass_back(last - 2)
    pass_back(last - 1)
    pass_back(last)

    @pl.when(end)
    def _():
        finish_d(0)
        lax.fori_loop(0, steps, finish, 0)

    finish_d(1)
    lax.fori_loop(steps, 2 * steps, finish, 0)

    for n in range(9):

        @pl.when(end)
        def _():
            lend(n).wait_recv()

        @pl.when(mid)
        def _():
            lend(n).wait_send()


    def sent(k, _):
        @pl.when(end)
        def _():
            for q in (3, 2, 1):
                from_end(k, q).wait_send()

        @pl.when(mid)
        def _():
            across(k, 3).wait_send()
            across(k, 2).wait_send()
            to_end(k).wait_send()

        return 0

    lax.fori_loop(0, 2 * steps, sent, 0)
    for p in range(2):

        @pl.when(end)
        def _():
            for u in range(2):
                for q in (3, 2, 1):
                    from_end_d(p, q, u).wait_send()

        @pl.when(mid)
        def _():
            for u in range(2):
                across_d(p, 3, u).wait_send()
                across_d(p, 2, u).wait_send()
                to_end_d(p, u).wait_send()


def gradients(x, dy, wg, wu, wd, moments):
    T, D = x.shape
    L, _, FF = wg.shape
    n = L * (FF // CHUNK)
    RG, RD = D // 8, FF // 8
    V, DMA = pltpu.VMEM, pltpu.SemaphoreType.DMA
    piece = (2, RG, CHUNK)
    return pl.pallas_call(
        functools.partial(gradients_kernel, T, D, FF),
        out_shape=[
            V((L, RG, FF), BF16),
            V((L, RG, FF), BF16),
            V((L, RD, D), BF16),
            *(pltpu.HBM(a.shape[1:], F32) for a in moments),
            *(pltpu.HBM(a.shape[1:], BF16) for a in moments[:3]),
        ],
        in_specs=[pl.BlockSpec(memory_space=pl.ANY)] * 11,
        out_specs=[pl.BlockSpec(memory_space=pltpu.VMEM)] * 3 + [pl.BlockSpec(memory_space=pltpu.HBM)] * 9,
        scratch_shapes=[
            V((T, D), BF16), V((T, D), BF16), V((T, D), BF16), V((D, T), BF16), V((T, D), BF16), V((T, D), F32),
            V((T, CHUNK), BF16), V((T, CHUNK), BF16), V((T, CHUNK), BF16),
            V((2, D, CHUNK), BF16), V((2, D, CHUNK), BF16), V((2, CHUNK, D), BF16),
            V((4, 4, 2, *piece), BF16), V((n, 4, *piece), BF16), V((n, *piece), F32),
            V((n, 3, *piece), BF16), V((n, 2, *piece), BF16),
            V((L, FF, D), BF16), V((L, 4, RD, D), BF16), V((L, RD, D), F32),
            V((L, 3, RD, D), BF16), V((L, 2, RD, D), BF16),
            DMA((2, 3)), DMA((1,)), DMA((n,)), DMA((n,)), DMA((n, 3)), DMA((n, 3)), DMA((n,)), DMA((n, 2)),
            DMA((L, 4)), DMA((L, 4)), DMA((L, 3, 2)), DMA((L, 3, 2)), DMA((L, 2)), DMA((L, 2, 2)), DMA((9,)), DMA((9,)), DMA((T // min(512, T),)),
        ],
        compiler_params=pltpu.CompilerParams(collective_id=0, has_side_effects=True, vmem_limit_bytes=VMEM_LIMIT - 5_000_000),
        name="gradients",
    )(x, dy, wg, wu, wd, *moments)


def update_kernel(count, *refs):
    g_s, m_hbm, v_hbm, w_hbm, lent = refs[0:3], refs[3:6], refs[6:9], refs[9:12], refs[12:21]
    w_out, m_out, v_out, refs = refs[21:24], refs[24:27], refs[27:30], refs[30:]
    m_s, v_s, w_s, n_s, refs = refs[0:3], refs[3:6], refs[6:9], refs[9:12], refs[12:]
    g_n, m_n, v_n, w_n, n_n, refs = refs[0:3], refs[3:6], refs[6:9], refs[9:12], refs[12:15], refs[15:]
    sq, in_sem, sq_send, sq_recv, r_send, r_recv, l_send, l_recv, p_send, p_recv, own_sem, mv_sem, near_sem = refs
    me, z, c, h, end = placed()
    partner = z * 2 + 1 - c
    L = 2
    parts = [(l, t) for l in (0, 1) for t in (2, 0, 1)]
    inward = z + 1 - 2 * h

    loads = []
    for t in range(3):
        block = pl.ds(pl.multiple_of(me * g_s[t].shape[1], 32), g_s[t].shape[1])
        loads.append([
            pltpu.make_async_copy(m_hbm[t], m_s[t], in_sem.at[t, 0]),
            pltpu.make_async_copy(v_hbm[t], v_s[t], in_sem.at[t, 1]),
            pltpu.make_async_copy(w_hbm[t].at[:, block], w_s[t], in_sem.at[t, 2]),
        ])
    for which in range(3):
        for t in (2, 0, 1):
            loads[t][which].start()

    near = []
    for t in range(3):
        block = pl.ds(pl.multiple_of((2 * inward + c) * g_s[t].shape[1], 32), g_s[t].shape[1])
        near += [
            pltpu.make_async_copy(lent[t], m_n[t], near_sem.at[t, 0]),
            pltpu.make_async_copy(lent[3 + t], v_n[t], near_sem.at[t, 1]),
            pltpu.make_async_copy(lent[6 + t], g_n[t], near_sem.at[t, 2]),
            pltpu.make_async_copy(w_hbm[t].at[1, block], w_n[t], near_sem.at[t, 3]),
        ]

    @pl.when(end)
    def _():
        for copy in near:
            copy.start()

    barrier = pltpu.get_barrier_semaphore()
    for other in range(1, 8):
        pl.semaphore_signal(barrier, inc=1, device_id={"dp": (me + other) % 8}, device_id_type=MESH)

    STEP = 16

    def strip(r):
        return pl.ds(pl.multiple_of(r * STEP, STEP), STEP)

    total = jnp.zeros((8, 128), F32)
    for t in range(3):
        R, C = g_s[t].shape[1:]

        def squares(r, total, t=t, R=R, C=C):
            l, q = r // (R // STEP), r % (R // STEP)
            g = g_s[t][l, strip(q)].astype(F32)
            return total + jnp.sum((g * g).reshape(STEP // 8, 8, C // 128, 128), axis=(0, 2))

        total = lax.fori_loop(0, L * (R // STEP), squares, total)
    sq[me] = total
    pl.semaphore_wait(barrier, 7)

    def tell(other):
        to = (me + other) % 8
        return remote(sq.at[me], sq.at[me], sq_send.at[other], sq_recv.at[8 - other], to)

    def told(other):
        src = (me + other) % 8
        return remote(sq.at[src], sq.at[src], sq_send.at[8 - other], sq_recv.at[other], me)

    for other in range(1, 8):
        tell(other).start()
    for t in range(3):
        for which in range(3):
            loads[t][which].wait()
    for other in range(1, 8):
        told(other).wait_recv()
    for other in range(1, 8):
        tell(other).wait_send()
    whole = jnp.full((8, 128), jnp.sum(sq[...]), F32)
    factor = jnp.minimum(1.0, 0.5 * lax.rsqrt(whole / count + 1e-30))[0:1, 0:1]

    def block(p, zt, ct):
        l, t = parts[p]
        R = g_s[t].shape[1]
        return w_out[t].at[l, pl.ds(pl.multiple_of((2 * zt + ct) * R, 32), R)]

    def mine(p):
        l, t = parts[p]
        return n_s[t].at[l]

    def to_right(p, hop):
        src = mine(p) if hop == 0 else block(p, z - hop, c)
        return remote(src, block(p, z - hop, c), r_send.at[p, hop], r_recv.at[p, hop], (z + 1) * 2 + c)

    def to_left(p, hop):
        src = mine(p) if hop == 0 else block(p, z + hop, c)
        return remote(src, block(p, z + hop, c), l_send.at[p, hop], l_recv.at[p, hop], (z - 1) * 2 + c)

    def to_partner(p, zt, own=False):
        return remote(mine(p) if own else block(p, zt, c), block(p, zt, c), p_send.at[p, zt], p_recv.at[p, zt], partner)

    def keep(p):
        return pltpu.make_async_copy(mine(p), block(p, z, c), own_sem.at[p])

    def moments(p):
        l, t = parts[p]
        return (
            pltpu.make_async_copy(m_s[t].at[l], m_out[t].at[l], mv_sem.at[p, 0]),
            pltpu.make_async_copy(v_s[t].at[l], v_out[t].at[l], mv_sem.at[p, 1]),
        )

    def adamw(g, m, v, w):
        g, w = g.astype(F32) * factor, w.astype(F32)
        m = 0.9 * m + 0.1 * g
        v = 0.95 * v + 0.05 * g * g
        return (w - 0.02 * (m * lax.rsqrt(v + 1e-8) + 0.1 * w)).astype(BF16), m, v

    def sends_right(p, hop):
        if hop == 0 and parts[p][0] == 1:
            return jnp.logical_and(z < 3, z != 2)
        return jnp.logical_and(z < 3, z >= hop)

    def sends_left(p, hop):
        if hop == 0 and parts[p][0] == 1:
            return jnp.logical_and(z > 0, z != 1)
        return jnp.logical_and(z > 0, z + hop <= 3)

    for p, (l, t) in enumerate(parts):

        def own(r, _, l=l, t=t):
            at = strip(r)
            new, m, v = adamw(g_s[t][l, at], m_s[t][l, at], v_s[t][l, at], w_s[t][l, at])
            m_s[t][l, at] = m
            v_s[t][l, at] = v
            n_s[t][l, at] = new
            return 0

        lax.fori_loop(0, g_s[t].shape[1] // STEP, own, 0)

        @pl.when(sends_right(p, 0))
        def _():
            to_right(p, 0).start()

        @pl.when(sends_left(p, 0))
        def _():
            to_left(p, 0).start()

        to_partner(p, z, True).start()
        keep(p).start()
        for copy in moments(p):
            copy.start()

    def near_block(p):
        return block(p, inward, c)

    def near_keep(p):
        return pltpu.make_async_copy(n_n[parts[p][1]], near_block(p), own_sem.at[p])

    def near_to_partner(p):
        return remote(n_n[parts[p][1]], near_block(p), p_send.at[p, inward], p_recv.at[p, inward], partner)

    @pl.when(end)
    def _():
        for copy in near:
            copy.wait()
        for p, (l, t) in enumerate(parts):
            if l == 1:

                def neighbour(r, _, t=t):
                    at = strip(r)
                    n_n[t][at] = adamw(g_n[t][at], m_n[t][at], v_n[t][at], w_n[t][at])[0]
                    return 0

                lax.fori_loop(0, g_s[t].shape[1] // STEP, neighbour, 0)
                near_to_partner(p).start()
                keep(p).wait()
                near_keep(p).start()

    n = len(parts)
    for hop in range(3):
        for p in range(n):
            borrowed = hop == 0 and parts[p][0] == 1

            @pl.when(jnp.logical_and(z > hop, z != 3) if borrowed else z > hop)
            def _():
                to_right(p, hop).wait_recv()

                if hop < 2:

                    @pl.when(z < 3)
                    def _():
                        to_right(p, hop + 1).start()

                to_partner(p, z - hop - 1).start()

            @pl.when(jnp.logical_and(z + hop < 3, z != 0) if borrowed else z + hop < 3)
            def _():
                to_left(p, hop).wait_recv()

                if hop < 2:

                    @pl.when(z > 0)
                    def _():
                        to_left(p, hop + 1).start()

                to_partner(p, z + hop + 1).start()

    for p in range(n):
        for zt in range(4):
            to_partner(p, zt).wait_recv()
    for p in range(n):
        keep(p).wait()
        for copy in moments(p):
            copy.wait()
        for zt in range(4):
            to_partner(p, zt).wait_send()
        for hop in range(3):

            @pl.when(sends_right(p, hop))
            def _():
                to_right(p, hop).wait_send()

            @pl.when(sends_left(p, hop))
            def _():
                to_left(p, hop).wait_send()


def update(g, m, v, w, lent):
    V, DMA = pltpu.VMEM, pltpu.SemaphoreType.DMA
    S = jax.ShapeDtypeStruct
    count = 8 * sum(a.size for a in g)
    out = [V(a.shape, BF16) for a in w] + [V(a.shape, F32) for a in (*m, *v)]
    return pl.pallas_call(
        functools.partial(update_kernel, float(count)),
        out_shape=out,
        in_specs=[pl.BlockSpec(memory_space=pltpu.VMEM)] * 3 + [pl.BlockSpec(memory_space=pltpu.HBM)] * 18,
        out_specs=[pl.BlockSpec(memory_space=pl.ANY)] * 9,
        scratch_shapes=[
            *(V(a.shape, F32) for a in m), *(V(a.shape, F32) for a in v),
            *(V(a.shape, BF16) for a in g), *(V(a.shape, BF16) for a in g),
            *(V(a.shape[1:], BF16) for a in g), *(V(a.shape[1:], F32) for a in m), *(V(a.shape[1:], F32) for a in v),
            *(V(a.shape[1:], BF16) for a in g), *(V(a.shape[1:], BF16) for a in g),
            V((8, 8, 128), F32), DMA((3, 3)), DMA((8,)), DMA((8,)),
            DMA((6, 3)), DMA((6, 3)), DMA((6, 3)), DMA((6, 3)), DMA((6, 4)), DMA((6, 4)), DMA((6,)), DMA((6, 2)), DMA((3, 4)),
        ],
        compiler_params=pltpu.CompilerParams(collective_id=1, has_side_effects=True, vmem_limit_bytes=36_000_000),
        name="update",
    )(*(pltpu.with_memory_space_constraint(a, pltpu.VMEM) for a in g), *m, *v, *w, *lent)


def store_kernel(*refs):
    n = len(refs) // 2
    src, dst, sem = refs[:n], refs[n : 2 * n], refs[2 * n]
    copies = [pltpu.make_async_copy(src[i].at[l], dst[i].at[l], sem.at[i, l]) for i in range(n) for l in range(2)]
    for copy in copies:
        copy.start()
    for copy in copies:
        copy.wait()


def store(arrays):
    n = len(arrays)
    return pl.pallas_call(
        store_kernel,
        out_shape=[jax.ShapeDtypeStruct(a.shape, a.dtype) for a in arrays],
        in_specs=[pl.BlockSpec(memory_space=pl.ANY)] * n,
        out_specs=[pl.BlockSpec(memory_space=pltpu.HBM)] * n,
        scratch_shapes=[pltpu.SemaphoreType.DMA((n, 2))],
        compiler_params=pltpu.CompilerParams(vmem_limit_bytes=1_000_000),
        name="store",
    )(*arrays)


def solution(mesh):
    def step(x, dy, *arrays):
        w, m, v = (arrays[i : i + 3] for i in (0, 3, 6))
        out = gradients(x[0], dy[0], *w, (*m, *v))
        return tuple(store(update(out[:3], m, v, w, out[3:])))

    whole, split = P(None, None, None), P(None, "dp", None)
    return jax.shard_map(
        step,
        mesh=mesh,
        in_specs=(P(("rep", "dp")),) * 2 + (whole,) * 3 + (split,) * 6,
        out_specs=(P("rep", None, None),) * 3 + (P("rep", "dp", None),) * 6,
        check_vma=False,
    )
```

```python
import functools

import jax
import jax.numpy as jnp
from jax import lax
from jax.experimental import pallas as pl
from jax.experimental.pallas import tpu as pltpu
from jax.sharding import PartitionSpec as P

F32, BF16 = jnp.float32, jnp.bfloat16
MESH = pl.DeviceIdType.MESH
VMEM_LIMIT = 67_043_328
CHUNK = 256


def dot(a, b, ca=1, cb=0):
    return lax.dot_general(a, b, (((ca,), (cb,)), ((), ())), preferred_element_type=F32)


def placed():
    me = lax.axis_index("dp")
    z, c = me // 2, me % 2
    h = z // 2
    end = (z + h) % 2 == 0
    return me, z, c, h, end


def remote(src, dst, send, recv, to):
    return pltpu.make_async_remote_copy(
        src_ref=src, dst_ref=dst, send_sem=send, recv_sem=recv, device_id={"dp": to}, device_id_type=MESH
    )


def gradients_kernel(
    T, D, FF, x_hbm, dy_hbm, wg_hbm, wu_hbm, wd_hbm, *refs
):
    moments, (gg_ref, gu_ref, gd_ref), lent = refs[:6], refs[6:9], refs[9:18]
    (
    H, A0, A1, AT, DY, ACC, hid, dg, du, wgs, wus, wds,
    own, prec, fin, RE, RM, ownd, precd, find, REd, RMd,
    w_sem, in_sem, d_send, d_recv, e_send, e_recv, m_send, m_recv,
    dd_send, dd_recv, ed_send, ed_recv, md_send, md_recv, lend_send, lend_recv, x_sem,
    ) = refs[18:]
    me, z, c, h, end = placed()
    partner = z * 2 + 1 - c
    d = 1 - 2 * h
    inward, outward = (z + d) * 2 + c, (z - d) * 2 + c
    mid = jnp.logical_not(end)
    TT = min(512, T)
    tiles = T // TT
    steps = FF // CHUNK
    RG, RD = D // 8, FF // 8

    def target(q):
        return q + h * (3 - 2 * q)

    def column(i):
        return (i + steps - 2) % steps

    def rows(t):
        return pl.ds(pl.multiple_of(t * TT, TT), TT)

    TB = min(1024, T)

    def big(t):
        return pl.ds(pl.multiple_of(t * TB, TB), TB)

    def weights(l, i, s):
        cols = pl.ds(pl.multiple_of(column(i) * CHUNK, CHUNK), CHUNK)
        slot = s % 2
        return (
            pltpu.make_async_copy(wg_hbm.at[l, :, cols], wgs.at[slot], w_sem.at[slot, 0]),
            pltpu.make_async_copy(wu_hbm.at[l, :, cols], wus.at[slot], w_sem.at[slot, 1]),
            pltpu.make_async_copy(wd_hbm.at[l, cols, :], wds.at[slot], w_sem.at[slot, 2]),
        )

    def get_x(t):
        return pltpu.make_async_copy(x_hbm.at[rows(t)], H.at[rows(t)], x_sem.at[t])

    get_dy = pltpu.make_async_copy(dy_hbm, DY, in_sem.at[0])
    for t in range(tiles):
        get_x(t).start()
    for copy in weights(0, 0, 0):
        copy.start()
    get_dy.start()

    barrier = pltpu.get_barrier_semaphore()
    pl.semaphore_signal(barrier, inc=1, device_id={"dp": partner}, device_id_type=MESH)
    pl.semaphore_signal(barrier, inc=1, device_id={"dp": inward}, device_id_type=MESH)

    @pl.when(mid)
    def _():
        pl.semaphore_signal(barrier, inc=1, device_id={"dp": outward}, device_id_type=MESH)

    def lend(n):
        src = moments[n].at[1] if n < 6 else (gg_ref, gu_ref, gd_ref)[n - 6].at[1]
        return remote(src, lent[n], lend_send.at[n], lend_recv.at[n], outward)

    def normed(wide):
        return wide * lax.rsqrt(jnp.mean(wide * wide, -1, keepdims=True) + 1e-6)

    def first(t, _):
        get_x(t).wait()
        A0[rows(t)] = normed(H[rows(t)].astype(F32)).astype(BF16)
        ACC[rows(t)] = jnp.zeros((TT, D), F32)
        return 0

    lax.fori_loop(0, tiles, first, 0)

    @pl.when(mid)
    def _():
        pl.semaphore_wait(barrier, 3)
        for n in range(6):
            lend(n).start()

    @pl.when(end)
    def _():
        pl.semaphore_wait(barrier, 2)


    def next_weights(l, i, s, after):
        for copy in weights(l, i, s):
            copy.wait()

        @pl.when(i < steps - 1)
        def _():
            for copy in weights(l, i + 1, s + 1):
                copy.start()

        if after is not None:

            @pl.when(i == steps - 1)
            def _():
                for copy in weights(after, 0, s + 1):
                    copy.start()

    def forward(i, _):
        next_weights(0, i, i, 1)
        slot = i % 2

        def tile(t, _):
            a = A0[big(t)]
            gate, up = dot(a, wgs[slot]), dot(a, wus[slot])
            hidden = (gate * lax.logistic(gate) * up).astype(BF16)
            down = dot(hidden, wds[slot])

            ACC[big(t)] += down
            return 0

        lax.fori_loop(0, T // TB, tile, 0)
        return 0

    lax.fori_loop(0, steps, forward, 0)

    def between(t, _):
        out = ACC[rows(t)].astype(BF16).astype(F32)
        ACC[rows(t)] = jnp.zeros((TT, D), F32)
        h1 = (H[rows(t)].astype(F32) + out).astype(BF16)
        H[rows(t)] = h1
        a = normed(h1.astype(F32)).astype(BF16)
        A1[rows(t)] = a
        AT[:, rows(t)] = a.T
        return 0

    lax.fori_loop(0, tiles, between, 0)
    get_dy.wait()

    def to_partner(k):
        return remote(own.at[k % 4, :, 1 - c], prec.at[k], d_send.at[k], d_recv.at[k], partner)

    def to_partner_d(p, zt):
        block = pl.ds(pl.multiple_of((2 * zt + 1 - c) * RD, RD), RD)
        return remote(ownd.at[p, block], precd.at[p, zt], dd_send.at[p, zt], dd_recv.at[p, zt], partner)

    def from_end(k, q):
        return remote(prec.at[k, target(q)], RE.at[k, q - 1], e_send.at[k, q - 1], e_recv.at[k, q - 1], inward)

    def across(k, q):
        return remote(prec.at[k, target(q)], RM.at[k, 3 - q], e_send.at[k, q - 1], m_recv.at[k, 3 - q], inward)

    def to_end(k):
        return remote(prec.at[k, target(0)], RM.at[k, 0], m_send.at[k], m_recv.at[k, 0], outward)

    def half(u):
        return pl.ds(u * (RD // 2), RD // 2)

    def from_end_d(p, q, u):
        src, dst = precd.at[p, target(q), half(u)], REd.at[p, q - 1, half(u)]
        return remote(src, dst, ed_send.at[p, q - 1, u], ed_recv.at[p, q - 1, u], inward)

    def across_d(p, q, u):
        src, dst = precd.at[p, target(q), half(u)], RMd.at[p, 3 - q, half(u)]
        return remote(src, dst, ed_send.at[p, q - 1, u], md_recv.at[p, 3 - q, u], inward)

    def to_end_d(p, u):
        src, dst = precd.at[p, target(0), half(u)], RMd.at[p, 0, half(u)]
        return remote(src, dst, md_send.at[p, u], md_recv.at[p, 0, u], outward)

    def both(k, zt):
        return own[k % 4, zt, c].astype(F32) + prec[k, zt].astype(F32)

    def both_d(p, zt, u):
        block = pl.ds(pl.multiple_of((2 * zt + c) * RD + u * (RD // 2), RD // 2), RD // 2)
        return ownd[p, block].astype(F32) + precd[p, zt, half(u)].astype(F32)

    def share(k):
        to_partner(k).wait()
        fin[k] = both(k, z)

        @pl.when(end)
        def _():
            for q in (3, 2, 1):
                prec[k, target(q)] = both(k, target(q)).astype(BF16)
                from_end(k, q).start()

    def share_d(p, zt):
        to_partner_d(p, zt).wait()
        q = zt + h * (3 - 2 * zt)

        @pl.when(zt == z)
        def _():
            for u in range(2):
                find[p, half(u)] = both_d(p, zt, u)

        @pl.when(jnp.logical_and(end, zt != z))
        def _():
            for u in range(2):
                precd[p, zt, half(u)] = both_d(p, zt, u).astype(BF16)
                from_end_d(p, q, u).start()

    def pass_on(k):
        @pl.when(mid)
        def _():
            for q in (3, 2):
                from_end(k, q).wait_recv()
                prec[k, target(q)] = (both(k, target(q)) + RE[k, q - 1].astype(F32)).astype(BF16)
                across(k, q).start()

    def pass_back(k):
        @pl.when(mid)
        def _():
            across(k, 3).wait_recv()
            prec[k, target(0)] = (both(k, target(0)) + RM[k, 0].astype(F32)).astype(BF16)
            to_end(k).start()

    def pass_on_d(p, q, u):
        @pl.when(mid)
        def _():
            from_end_d(p, q, u).wait_recv()
            total = both_d(p, target(q), u) + REd[p, q - 1, half(u)].astype(F32)
            precd[p, target(q), half(u)] = total.astype(BF16)
            across_d(p, q, u).start()

    def pass_back_d(p):
        @pl.when(mid)
        def _():
            for u in range(2):
                across_d(p, 3, u).wait_recv()
                total = both_d(p, target(0), u) + RMd[p, 0, half(u)].astype(F32)
                precd[p, target(0), half(u)] = total.astype(BF16)
                to_end_d(p, u).start()

    def finish(k, _):
        p, i = k // steps, k % steps
        l = 1 - p
        cols = pl.ds(pl.multiple_of(column(i) * CHUNK, CHUNK), CHUNK)

        def put(total):
            gg_ref[l, :, cols] = total[0].astype(BF16)
            gu_ref[l, :, cols] = total[1].astype(BF16)

        @pl.when(end)
        def _():
            to_end(k).wait_recv()
            put(fin[k] + RM[k, 0].astype(F32))

        @pl.when(mid)
        def _():
            from_end(k, 1).wait_recv()
            across(k, 2).wait_recv()
            put(fin[k] + RE[k, 0].astype(F32) + RM[k, 1].astype(F32))

        return 0

    def finish_d(p):
        @pl.when(end)
        def _():
            for u in range(2):
                to_end_d(p, u).wait_recv()
            gd_ref[1 - p] = (find[p] + RMd[p, 0].astype(F32)).astype(BF16)

        @pl.when(mid)
        def _():
            for u in range(2):
                from_end_d(p, 1, u).wait_recv()
                across_d(p, 2, u).wait_recv()
            gd_ref[1 - p] = (find[p] + REd[p, 0].astype(F32) + RMd[p, 1].astype(F32)).astype(BF16)

    def backward(p, A, i, _):
        l = 1 - p
        s = steps * (1 + p) + i
        k = steps * p + i
        slot = s % 2
        j = column(i)
        next_weights(l, i, s, 0 if p == 0 else None)

        def tile(t, _):
            a = A[big(t)]
            gate, up = dot(a, wgs[slot]), dot(a, wus[slot])
            dh = dot(DY[big(t)], wds[slot], 1, 1).astype(BF16).astype(F32)
            sig = lax.logistic(gate)
            act = gate * sig
            hid[big(t)] = (act * up).astype(BF16)
            du[big(t)] = (dh * act).astype(BF16)
            dg[big(t)] = (dh * up * (sig * (1.0 + gate * (1.0 - sig)))).astype(BF16)
            return 0

        lax.fori_loop(0, T // TB, tile, 0)
        here = pl.ds(pl.multiple_of(j * CHUNK, CHUNK), CHUNK)
        own[k % 4, :, :, 0] = dot(AT[...], dg[...]).astype(BF16).reshape(4, 2, RG, CHUNK)
        own[k % 4, :, :, 1] = dot(AT[...], du[...]).astype(BF16).reshape(4, 2, RG, CHUNK)
        to_partner(k).start()
        ownd[p, here] = dot(hid[...], DY[...], 0, 0).astype(BF16)
        zt = (i // 2 + 3) % 4
        down_ready = jnp.logical_or(i % 2 == 1, i == steps - 1)

        @pl.when(down_ready)
        def _():
            to_partner_d(p, zt).start()

        if p == 0:

            @pl.when(i == 0)
            def _():
                share(k)

            def back(t, _):
                da = dot(dg[big(t)], wgs[slot], 1, 1) + dot(du[big(t)], wus[slot], 1, 1)
                ACC[big(t)] += da
                return 0

            lax.fori_loop(0, T // TB, back, 0)

        @pl.when(down_ready)
        def _():
            share_d(p, zt)

        @pl.when(k > 0)
        def _():
            share(k)

        @pl.when(k >= 2)
        def _():
            pass_on(k - 2)

        @pl.when(k >= 3)
        def _():
            pass_back(k - 3)

        if p == 1:

            @pl.when(i == 2)
            def _():
                for q in (3, 2):
                    for u in range(2):
                        pass_on_d(0, q, u)
                pass_back_d(0)

            @pl.when(jnp.logical_and(mid, i == 3))
            def _():
                finish_d(0)
                lax.fori_loop(0, steps, finish, 0)
                for n in range(6, 9):
                    lend(n).start()

        return 0

    lax.fori_loop(0, steps, functools.partial(backward, 0, A1), 0)

    def through_norm(t, _):
        da = ACC[rows(t)].astype(BF16).astype(F32)
        wide = H[rows(t)].astype(F32)
        scale = lax.rsqrt(jnp.mean(wide * wide, -1, keepdims=True) + 1e-6)
        along = jnp.mean(da * wide, -1, keepdims=True)
        dh = (da * scale - wide * (scale * scale * scale * along)).astype(BF16).astype(F32)
        DY[rows(t)] = (DY[rows(t)].astype(F32) + dh).astype(BF16)
        AT[:, rows(t)] = A0[rows(t)].T
        return 0

    lax.fori_loop(0, tiles, through_norm, 0)
    lax.fori_loop(0, steps, functools.partial(backward, 1, A0), 0)

    last = 2 * steps - 1
    pass_on_d(1, 3, 0)
    pass_on_d(1, 3, 1)
    pass_on(last - 1)
    pass_on_d(1, 2, 0)
    pass_on(last)
    pass_on_d(1, 2, 1)
    pass_back_d(1)
    pass_back(last - 2)
    pass_back(last - 1)
    pass_back(last)

    @pl.when(end)
    def _():
        finish_d(0)
        lax.fori_loop(0, steps, finish, 0)

    finish_d(1)
    lax.fori_loop(steps, 2 * steps, finish, 0)

    for n in range(9):

        @pl.when(end)
        def _():
            lend(n).wait_recv()

        @pl.when(mid)
        def _():
            lend(n).wait_send()


    def sent(k, _):
        @pl.when(end)
        def _():
            for q in (3, 2, 1):
                from_end(k, q).wait_send()

        @pl.when(mid)
        def _():
            across(k, 3).wait_send()
            across(k, 2).wait_send()
            to_end(k).wait_send()

        return 0

    lax.fori_loop(0, 2 * steps, sent, 0)
    for p in range(2):

        @pl.when(end)
        def _():
            for u in range(2):
                for q in (3, 2, 1):
                    from_end_d(p, q, u).wait_send()

        @pl.when(mid)
        def _():
            for u in range(2):
                across_d(p, 3, u).wait_send()
                across_d(p, 2, u).wait_send()
                to_end_d(p, u).wait_send()


def gradients(x, dy, wg, wu, wd, moments):
    T, D = x.shape
    L, _, FF = wg.shape
    n = L * (FF // CHUNK)
    RG, RD = D // 8, FF // 8
    V, DMA = pltpu.VMEM, pltpu.SemaphoreType.DMA
    piece = (2, RG, CHUNK)
    return pl.pallas_call(
        functools.partial(gradients_kernel, T, D, FF),
        out_shape=[
            V((L, RG, FF), BF16),
            V((L, RG, FF), BF16),
            V((L, RD, D), BF16),
            *(pltpu.HBM(a.shape[1:], F32) for a in moments),
            *(pltpu.HBM(a.shape[1:], BF16) for a in moments[:3]),
        ],
        in_specs=[pl.BlockSpec(memory_space=pl.ANY)] * 11,
        out_specs=[pl.BlockSpec(memory_space=pltpu.VMEM)] * 3 + [pl.BlockSpec(memory_space=pltpu.HBM)] * 9,
        scratch_shapes=[
            V((T, D), BF16), V((T, D), BF16), V((T, D), BF16), V((D, T), BF16), V((T, D), BF16), V((T, D), F32),
            V((T, CHUNK), BF16), V((T, CHUNK), BF16), V((T, CHUNK), BF16),
            V((2, D, CHUNK), BF16), V((2, D, CHUNK), BF16), V((2, CHUNK, D), BF16),
            V((4, 4, 2, *piece), BF16), V((n, 4, *piece), BF16), V((n, *piece), F32),
            V((n, 3, *piece), BF16), V((n, 2, *piece), BF16),
            V((L, FF, D), BF16), V((L, 4, RD, D), BF16), V((L, RD, D), F32),
            V((L, 3, RD, D), BF16), V((L, 2, RD, D), BF16),
            DMA((2, 3)), DMA((1,)), DMA((n,)), DMA((n,)), DMA((n, 3)), DMA((n, 3)), DMA((n,)), DMA((n, 2)),
            DMA((L, 4)), DMA((L, 4)), DMA((L, 3, 2)), DMA((L, 3, 2)), DMA((L, 2)), DMA((L, 2, 2)), DMA((9,)), DMA((9,)), DMA((T // min(512, T),)),
        ],
        compiler_params=pltpu.CompilerParams(collective_id=0, has_side_effects=True, vmem_limit_bytes=VMEM_LIMIT - 2_300_000),
        name="gradients",
    )(x, dy, wg, wu, wd, *moments)


def update_kernel(count, *refs):
    g_s, m_hbm, v_hbm, w_hbm, lent = refs[0:3], refs[3:6], refs[6:9], refs[9:12], refs[12:21]
    w_out, m_out, v_out, refs = refs[21:24], refs[24:27], refs[27:30], refs[30:]
    m_s, v_s, w_s, n_s, refs = refs[0:3], refs[3:6], refs[6:9], refs[9:12], refs[12:]
    g_n, m_n, v_n, w_n, n_n, refs = refs[0:3], refs[3:6], refs[6:9], refs[9:12], refs[12:15], refs[15:]
    sq, in_sem, sq_send, sq_recv, r_send, r_recv, l_send, l_recv, p_send, p_recv, own_sem, mv_sem, near_sem = refs
    me, z, c, h, end = placed()
    partner = z * 2 + 1 - c
    L = 2
    parts = [(l, t) for l in (0, 1) for t in (2, 0, 1)]
    inward = z + 1 - 2 * h

    loads = []
    for t in range(3):
        block = pl.ds(pl.multiple_of(me * g_s[t].shape[1], 32), g_s[t].shape[1])
        loads.append([
            pltpu.make_async_copy(m_hbm[t], m_s[t], in_sem.at[t, 0]),
            pltpu.make_async_copy(v_hbm[t], v_s[t], in_sem.at[t, 1]),
            pltpu.make_async_copy(w_hbm[t].at[:, block], w_s[t], in_sem.at[t, 2]),
        ])
    for which in range(3):
        for t in (2, 0, 1):
            loads[t][which].start()

    near = []
    for t in range(3):
        block = pl.ds(pl.multiple_of((2 * inward + c) * g_s[t].shape[1], 32), g_s[t].shape[1])
        near += [
            pltpu.make_async_copy(lent[t], m_n[t], near_sem.at[t, 0]),
            pltpu.make_async_copy(lent[3 + t], v_n[t], near_sem.at[t, 1]),
            pltpu.make_async_copy(lent[6 + t], g_n[t], near_sem.at[t, 2]),
            pltpu.make_async_copy(w_hbm[t].at[1, block], w_n[t], near_sem.at[t, 3]),
        ]

    @pl.when(end)
    def _():
        for copy in near:
            copy.start()

    barrier = pltpu.get_barrier_semaphore()
    for other in range(1, 8):
        pl.semaphore_signal(barrier, inc=1, device_id={"dp": (me + other) % 8}, device_id_type=MESH)

    STEP = 16

    def strip(r):
        return pl.ds(pl.multiple_of(r * STEP, STEP), STEP)

    total = jnp.zeros((8, 128), F32)
    for t in range(3):
        R, C = g_s[t].shape[1:]

        def squares(r, total, t=t, R=R, C=C):
            l, q = r // (R // STEP), r % (R // STEP)
            g = g_s[t][l, strip(q)].astype(F32)
            return total + jnp.sum((g * g).reshape(STEP // 8, 8, C // 128, 128), axis=(0, 2))

        total = lax.fori_loop(0, L * (R // STEP), squares, total)
    sq[me] = total
    pl.semaphore_wait(barrier, 7)

    def tell(other):
        to = (me + other) % 8
        return remote(sq.at[me], sq.at[me], sq_send.at[other], sq_recv.at[8 - other], to)

    def told(other):
        src = (me + other) % 8
        return remote(sq.at[src], sq.at[src], sq_send.at[8 - other], sq_recv.at[other], me)

    for other in range(1, 8):
        tell(other).start()
    for t in range(3):
        for which in range(3):
            loads[t][which].wait()
    for other in range(1, 8):
        told(other).wait_recv()
    for other in range(1, 8):
        tell(other).wait_send()
    whole = jnp.full((8, 128), jnp.sum(sq[...]), F32)
    factor = jnp.minimum(1.0, 0.5 * lax.rsqrt(whole / count + 1e-30))[0:1, 0:1]

    def block(p, zt, ct):
        l, t = parts[p]
        R = g_s[t].shape[1]
        return w_out[t].at[l, pl.ds(pl.multiple_of((2 * zt + ct) * R, 32), R)]

    def mine(p):
        l, t = parts[p]
        return n_s[t].at[l]

    def to_right(p, hop):
        src = mine(p) if hop == 0 else block(p, z - hop, c)
        return remote(src, block(p, z - hop, c), r_send.at[p, hop], r_recv.at[p, hop], (z + 1) * 2 + c)

    def to_left(p, hop):
        src = mine(p) if hop == 0 else block(p, z + hop, c)
        return remote(src, block(p, z + hop, c), l_send.at[p, hop], l_recv.at[p, hop], (z - 1) * 2 + c)

    def to_partner(p, zt, own=False):
        return remote(mine(p) if own else block(p, zt, c), block(p, zt, c), p_send.at[p, zt], p_recv.at[p, zt], partner)

    def keep(p):
        return pltpu.make_async_copy(mine(p), block(p, z, c), own_sem.at[p])

    def moments(p):
        l, t = parts[p]
        return (
            pltpu.make_async_copy(m_s[t].at[l], m_out[t].at[l], mv_sem.at[p, 0]),
            pltpu.make_async_copy(v_s[t].at[l], v_out[t].at[l], mv_sem.at[p, 1]),
        )

    def adamw(g, m, v, w):
        g, w = g.astype(F32) * factor, w.astype(F32)
        m = 0.9 * m + 0.1 * g
        v = 0.95 * v + 0.05 * g * g
        return (w - 0.02 * (m * lax.rsqrt(v + 1e-8) + 0.1 * w)).astype(BF16), m, v

    def sends_right(p, hop):
        if hop == 0 and parts[p][0] == 1:
            return jnp.logical_and(z < 3, z != 2)
        return jnp.logical_and(z < 3, z >= hop)

    def sends_left(p, hop):
        if hop == 0 and parts[p][0] == 1:
            return jnp.logical_and(z > 0, z != 1)
        return jnp.logical_and(z > 0, z + hop <= 3)

    for p, (l, t) in enumerate(parts):

        def own(r, _, l=l, t=t):
            at = strip(r)
            new, m, v = adamw(g_s[t][l, at], m_s[t][l, at], v_s[t][l, at], w_s[t][l, at])
            m_s[t][l, at] = m
            v_s[t][l, at] = v
            n_s[t][l, at] = new
            return 0

        lax.fori_loop(0, g_s[t].shape[1] // STEP, own, 0)

        @pl.when(sends_right(p, 0))
        def _():
            to_right(p, 0).start()

        @pl.when(sends_left(p, 0))
        def _():
            to_left(p, 0).start()

        to_partner(p, z, True).start()
        keep(p).start()
        for copy in moments(p):
            copy.start()

    def near_block(p):
        return block(p, inward, c)

    def near_keep(p):
        return pltpu.make_async_copy(n_n[parts[p][1]], near_block(p), own_sem.at[p])

    def near_to_partner(p):
        return remote(n_n[parts[p][1]], near_block(p), p_send.at[p, inward], p_recv.at[p, inward], partner)

    @pl.when(end)
    def _():
        for copy in near:
            copy.wait()
        for p, (l, t) in enumerate(parts):
            if l == 1:

                def neighbour(r, _, t=t):
                    at = strip(r)
                    n_n[t][at] = adamw(g_n[t][at], m_n[t][at], v_n[t][at], w_n[t][at])[0]
                    return 0

                lax.fori_loop(0, g_s[t].shape[1] // STEP, neighbour, 0)
                near_to_partner(p).start()
                keep(p).wait()
                near_keep(p).start()

    n = len(parts)
    for hop in range(3):
        for p in range(n):
            borrowed = hop == 0 and parts[p][0] == 1

            @pl.when(jnp.logical_and(z > hop, z != 3) if borrowed else z > hop)
            def _():
                to_right(p, hop).wait_recv()

                if hop < 2:

                    @pl.when(z < 3)
                    def _():
                        to_right(p, hop + 1).start()

                to_partner(p, z - hop - 1).start()

            @pl.when(jnp.logical_and(z + hop < 3, z != 0) if borrowed else z + hop < 3)
            def _():
                to_left(p, hop).wait_recv()

                if hop < 2:

                    @pl.when(z > 0)
                    def _():
                        to_left(p, hop + 1).start()

                to_partner(p, z + hop + 1).start()

    for p in range(n):
        for zt in range(4):
            to_partner(p, zt).wait_recv()
    for p in range(n):
        keep(p).wait()
        for copy in moments(p):
            copy.wait()
        for zt in range(4):
            to_partner(p, zt).wait_send()
        for hop in range(3):

            @pl.when(sends_right(p, hop))
            def _():
                to_right(p, hop).wait_send()

            @pl.when(sends_left(p, hop))
            def _():
                to_left(p, hop).wait_send()


def update(g, m, v, w, lent):
    V, DMA = pltpu.VMEM, pltpu.SemaphoreType.DMA
    S = jax.ShapeDtypeStruct
    count = 8 * sum(a.size for a in g)
    out = [V(a.shape, BF16) for a in w] + [V(a.shape, F32) for a in (*m, *v)]
    return pl.pallas_call(
        functools.partial(update_kernel, float(count)),
        out_shape=out,
        in_specs=[pl.BlockSpec(memory_space=pltpu.VMEM)] * 3 + [pl.BlockSpec(memory_space=pltpu.HBM)] * 18,
        out_specs=[pl.BlockSpec(memory_space=pl.ANY)] * 9,
        scratch_shapes=[
            *(V(a.shape, F32) for a in m), *(V(a.shape, F32) for a in v),
            *(V(a.shape, BF16) for a in g), *(V(a.shape, BF16) for a in g),
            *(V(a.shape[1:], BF16) for a in g), *(V(a.shape[1:], F32) for a in m), *(V(a.shape[1:], F32) for a in v),
            *(V(a.shape[1:], BF16) for a in g), *(V(a.shape[1:], BF16) for a in g),
            V((8, 8, 128), F32), DMA((3, 3)), DMA((8,)), DMA((8,)),
            DMA((6, 3)), DMA((6, 3)), DMA((6, 3)), DMA((6, 3)), DMA((6, 4)), DMA((6, 4)), DMA((6,)), DMA((6, 2)), DMA((3, 4)),
        ],
        compiler_params=pltpu.CompilerParams(collective_id=1, has_side_effects=True, vmem_limit_bytes=36_000_000),
        name="update",
    )(*(pltpu.with_memory_space_constraint(a, pltpu.VMEM) for a in g), *m, *v, *w, *lent)


def store_kernel(*refs):
    n = len(refs) // 2
    src, dst, sem = refs[:n], refs[n : 2 * n], refs[2 * n]
    copies = [pltpu.make_async_copy(src[i].at[l], dst[i].at[l], sem.at[i, l]) for i in range(n) for l in range(2)]
    for copy in copies:
        copy.start()
    for copy in copies:
        copy.wait()


def store(arrays):
    n = len(arrays)
    return pl.pallas_call(
        store_kernel,
        out_shape=[jax.ShapeDtypeStruct(a.shape, a.dtype) for a in arrays],
        in_specs=[pl.BlockSpec(memory_space=pl.ANY)] * n,
        out_specs=[pl.BlockSpec(memory_space=pltpu.HBM)] * n,
        scratch_shapes=[pltpu.SemaphoreType.DMA((n, 2))],
        compiler_params=pltpu.CompilerParams(vmem_limit_bytes=1_000_000),
        name="store",
    )(*arrays)


def solution(mesh):
    def step(x, dy, *arrays):
        w, m, v = (arrays[i : i + 3] for i in (0, 3, 6))
        out = gradients(x[0], dy[0], *w, (*m, *v))
        return tuple(store(update(out[:3], m, v, w, out[3:])))

    whole, split = P(None, None, None), P(None, "dp", None)
    return jax.shard_map(
        step,
        mesh=mesh,
        in_specs=(P(("rep", "dp")),) * 2 + (whole,) * 3 + (split,) * 6,
        out_specs=(P("rep", None, None),) * 3 + (P("rep", "dp", None),) * 6,
        check_vma=False,
    )
```

```python
import functools

import jax
import jax.numpy as jnp
from jax import lax
from jax.experimental import pallas as pl
from jax.experimental.pallas import tpu as pltpu
from jax.sharding import PartitionSpec as P

F32, BF16 = jnp.float32, jnp.bfloat16
MESH = pl.DeviceIdType.MESH
VMEM_LIMIT = 67_043_328
CHUNK = 256


def dot(a, b, ca=1, cb=0):
    return lax.dot_general(a, b, (((ca,), (cb,)), ((), ())), preferred_element_type=F32)


def placed():
    me = lax.axis_index("dp")
    z, c = me // 2, me % 2
    h = z // 2
    end = (z + h) % 2 == 0
    return me, z, c, h, end


def remote(src, dst, send, recv, to):
    return pltpu.make_async_remote_copy(
        src_ref=src, dst_ref=dst, send_sem=send, recv_sem=recv, device_id={"dp": to}, device_id_type=MESH
    )


def gradients_kernel(
    T, D, FF, x_hbm, dy_hbm, wg_hbm, wu_hbm, wd_hbm, *refs
):
    moments, (gg_ref, gu_ref, gd_ref), lent = refs[:6], refs[6:9], refs[9:18]
    (
    H, A0, A1, AT, DY, ACC, hid, dg, du, wgs, wus, wds,
    own, prec, fin, RE, RM, ownd, precd, find, REd, RMd,
    w_sem, in_sem, d_send, d_recv, e_send, e_recv, m_send, m_recv,
    dd_send, dd_recv, ed_send, ed_recv, md_send, md_recv, lend_send, lend_recv, x_sem,
    ) = refs[18:]
    me, z, c, h, end = placed()
    partner = z * 2 + 1 - c
    d = 1 - 2 * h
    inward, outward = (z + d) * 2 + c, (z - d) * 2 + c
    mid = jnp.logical_not(end)
    TT = min(512, T)
    tiles = T // TT
    steps = FF // CHUNK
    RG, RD = D // 8, FF // 8

    def target(q):
        return q + h * (3 - 2 * q)

    def column(i):
        return (i + steps - 2) % steps

    def rows(t):
        return pl.ds(pl.multiple_of(t * TT, TT), TT)

    TB = min(1024, T)

    def big(t):
        return pl.ds(pl.multiple_of(t * TB, TB), TB)

    def weights(l, i, s):
        cols = pl.ds(pl.multiple_of(column(i) * CHUNK, CHUNK), CHUNK)
        slot = s % 2
        return (
            pltpu.make_async_copy(wg_hbm.at[l, :, cols], wgs.at[slot], w_sem.at[slot, 0]),
            pltpu.make_async_copy(wu_hbm.at[l, :, cols], wus.at[slot], w_sem.at[slot, 1]),
            pltpu.make_async_copy(wd_hbm.at[l, cols, :], wds.at[slot], w_sem.at[slot, 2]),
        )

    def get_x(t):
        return pltpu.make_async_copy(x_hbm.at[rows(t)], H.at[rows(t)], x_sem.at[t])

    get_dy = pltpu.make_async_copy(dy_hbm, DY, in_sem.at[0])
    for t in range(tiles):
        get_x(t).start()
    for copy in weights(0, 0, 0):
        copy.start()
    get_dy.start()

    barrier = pltpu.get_barrier_semaphore()
    pl.semaphore_signal(barrier, inc=1, device_id={"dp": partner}, device_id_type=MESH)
    pl.semaphore_signal(barrier, inc=1, device_id={"dp": inward}, device_id_type=MESH)

    @pl.when(mid)
    def _():
        pl.semaphore_signal(barrier, inc=1, device_id={"dp": outward}, device_id_type=MESH)

    def lend(n):
        src = moments[n].at[1] if n < 6 else (gg_ref, gu_ref, gd_ref)[n - 6].at[1]
        return remote(src, lent[n], lend_send.at[n], lend_recv.at[n], outward)

    def normed(wide):
        return wide * lax.rsqrt(jnp.mean(wide * wide, -1, keepdims=True) + 1e-6)

    def first(t, _):
        get_x(t).wait()
        A0[rows(t)] = normed(H[rows(t)].astype(F32)).astype(BF16)
        ACC[rows(t)] = jnp.zeros((TT, D), F32)
        return 0

    lax.fori_loop(0, tiles, first, 0)

    @pl.when(mid)
    def _():
        pl.semaphore_wait(barrier, 3)
        for n in range(6):
            lend(n).start()

    @pl.when(end)
    def _():
        pl.semaphore_wait(barrier, 2)


    def next_weights(l, i, s, after):
        for copy in weights(l, i, s):
            copy.wait()

        @pl.when(i < steps - 1)
        def _():
            for copy in weights(l, i + 1, s + 1):
                copy.start()

        if after is not None:

            @pl.when(i == steps - 1)
            def _():
                for copy in weights(after, 0, s + 1):
                    copy.start()

    def forward(i, _):
        next_weights(0, i, i, 1)
        slot = i % 2

        def tile(t, _):
            a = A0[big(t)]
            gate, up = dot(a, wgs[slot]), dot(a, wus[slot])
            hidden = (gate * lax.logistic(gate) * up).astype(BF16)
            down = dot(hidden, wds[slot])

            ACC[big(t)] += down
            return 0

        lax.fori_loop(0, T // TB, tile, 0)
        return 0

    lax.fori_loop(0, steps, forward, 0)

    def between(t, _):
        out = ACC[rows(t)].astype(BF16).astype(F32)
        ACC[rows(t)] = jnp.zeros((TT, D), F32)
        h1 = (H[rows(t)].astype(F32) + out).astype(BF16)
        H[rows(t)] = h1
        a = normed(h1.astype(F32)).astype(BF16)
        A1[rows(t)] = a
        AT[:, rows(t)] = a.T
        return 0

    lax.fori_loop(0, tiles, between, 0)
    get_dy.wait()

    def to_partner(k):
        return remote(own.at[k % 4, :, 1 - c], prec.at[k], d_send.at[k], d_recv.at[k], partner)

    def to_partner_d(p, zt):
        block = pl.ds(pl.multiple_of((2 * zt + 1 - c) * RD, RD), RD)
        return remote(ownd.at[p, block], precd.at[p, zt], dd_send.at[p, zt], dd_recv.at[p, zt], partner)

    def from_end(k, q):
        return remote(prec.at[k, target(q)], RE.at[k, slot_of(q)], e_send.at[k, q - 1], e_recv.at[k, q - 1], inward)

    def slot_of(q):
        return target(q) - (1 - h)

    def all_from_end(k):
        return remote(prec.at[k, pl.ds(1 - h, 3)], RE.at[k], e_send.at[k, 0], e_recv.at[k, 0], inward)

    def across(k, q):
        return remote(prec.at[k, target(q)], RM.at[k, 3 - q], e_send.at[k, q - 1], m_recv.at[k, 3 - q], inward)

    def to_end(k):
        return remote(prec.at[k, target(0)], RM.at[k, 0], m_send.at[k], m_recv.at[k, 0], outward)

    def half(u):
        return pl.ds(u * (RD // 2), RD // 2)

    def from_end_d(p, q, u):
        src, dst = precd.at[p, target(q), half(u)], REd.at[p, q - 1, half(u)]
        return remote(src, dst, ed_send.at[p, q - 1, u], ed_recv.at[p, q - 1, u], inward)

    def across_d(p, q, u):
        src, dst = precd.at[p, target(q), half(u)], RMd.at[p, 3 - q, half(u)]
        return remote(src, dst, ed_send.at[p, q - 1, u], md_recv.at[p, 3 - q, u], inward)

    def to_end_d(p, u):
        src, dst = precd.at[p, target(0), half(u)], RMd.at[p, 0, half(u)]
        return remote(src, dst, md_send.at[p, u], md_recv.at[p, 0, u], outward)

    def both(k, zt):
        return own[k % 4, zt, c].astype(F32) + prec[k, zt].astype(F32)

    def both_d(p, zt, u):
        block = pl.ds(pl.multiple_of((2 * zt + c) * RD + u * (RD // 2), RD // 2), RD // 2)
        return ownd[p, block].astype(F32) + precd[p, zt, half(u)].astype(F32)

    def share(k):
        to_partner(k).wait()
        fin[k] = both(k, z)

        @pl.when(end)
        def _():
            for q in (3, 2, 1):
                prec[k, target(q)] = both(k, target(q)).astype(BF16)

            @pl.when(k < 2 * steps - 1)
            def _():
                all_from_end(k).start()

            @pl.when(k == 2 * steps - 1)
            def _():
                for q in (3, 2, 1):
                    from_end(k, q).start()

    def share_d(p, zt):
        to_partner_d(p, zt).wait()
        q = zt + h * (3 - 2 * zt)

        @pl.when(zt == z)
        def _():
            for u in range(2):
                find[p, half(u)] = both_d(p, zt, u)

        @pl.when(jnp.logical_and(end, zt != z))
        def _():
            for u in range(2):
                precd[p, zt, half(u)] = both_d(p, zt, u).astype(BF16)
                from_end_d(p, q, u).start()

    def pass_on(k, apart=False):
        @pl.when(mid)
        def _():
            if not apart:
                all_from_end(k).wait_recv()
            for q in (3, 2):
                if apart:
                    from_end(k, q).wait_recv()
                prec[k, target(q)] = (both(k, target(q)) + RE[k, slot_of(q)].astype(F32)).astype(BF16)
                across(k, q).start()

    def pass_back(k):
        @pl.when(mid)
        def _():
            across(k, 3).wait_recv()
            prec[k, target(0)] = (both(k, target(0)) + RM[k, 0].astype(F32)).astype(BF16)
            to_end(k).start()

    def pass_on_d(p, q, u):
        @pl.when(mid)
        def _():
            from_end_d(p, q, u).wait_recv()
            total = both_d(p, target(q), u) + REd[p, q - 1, half(u)].astype(F32)
            precd[p, target(q), half(u)] = total.astype(BF16)
            across_d(p, q, u).start()

    def pass_back_d(p):
        @pl.when(mid)
        def _():
            for u in range(2):
                across_d(p, 3, u).wait_recv()
                total = both_d(p, target(0), u) + RMd[p, 0, half(u)].astype(F32)
                precd[p, target(0), half(u)] = total.astype(BF16)
                to_end_d(p, u).start()

    def finish(k, _):
        p, i = k // steps, k % steps
        l = 1 - p
        cols = pl.ds(pl.multiple_of(column(i) * CHUNK, CHUNK), CHUNK)

        def put(total):
            gg_ref[l, :, cols] = total[0].astype(BF16)
            gu_ref[l, :, cols] = total[1].astype(BF16)

        @pl.when(end)
        def _():
            to_end(k).wait_recv()
            put(fin[k] + RM[k, 0].astype(F32))

        @pl.when(mid)
        def _():
            @pl.when(k == 2 * steps - 1)
            def _():
                from_end(k, 1).wait_recv()

            across(k, 2).wait_recv()
            put(fin[k] + RE[k, slot_of(1)].astype(F32) + RM[k, 1].astype(F32))

        return 0

    def finish_d(p):
        @pl.when(end)
        def _():
            for u in range(2):
                to_end_d(p, u).wait_recv()
            gd_ref[1 - p] = (find[p] + RMd[p, 0].astype(F32)).astype(BF16)

        @pl.when(mid)
        def _():
            for u in range(2):
                from_end_d(p, 1, u).wait_recv()
                across_d(p, 2, u).wait_recv()
            gd_ref[1 - p] = (find[p] + REd[p, 0].astype(F32) + RMd[p, 1].astype(F32)).astype(BF16)

    def backward(p, A, i, _):
        l = 1 - p
        s = steps * (1 + p) + i
        k = steps * p + i
        slot = s % 2
        j = column(i)
        next_weights(l, i, s, 0 if p == 0 else None)

        def tile(t, _):
            a = A[big(t)]
            gate, up = dot(a, wgs[slot]), dot(a, wus[slot])
            dh = dot(DY[big(t)], wds[slot], 1, 1).astype(BF16).astype(F32)
            sig = lax.logistic(gate)
            act = gate * sig
            hid[big(t)] = (act * up).astype(BF16)
            du[big(t)] = (dh * act).astype(BF16)
            dg[big(t)] = (dh * up * (sig * (1.0 + gate * (1.0 - sig)))).astype(BF16)
            return 0

        lax.fori_loop(0, T // TB, tile, 0)
        here = pl.ds(pl.multiple_of(j * CHUNK, CHUNK), CHUNK)
        own[k % 4, :, :, 0] = dot(AT[...], dg[...]).astype(BF16).reshape(4, 2, RG, CHUNK)
        own[k % 4, :, :, 1] = dot(AT[...], du[...]).astype(BF16).reshape(4, 2, RG, CHUNK)
        to_partner(k).start()
        ownd[p, here] = dot(hid[...], DY[...], 0, 0).astype(BF16)
        zt = (i // 2 + 3) % 4
        down_ready = jnp.logical_or(i % 2 == 1, i == steps - 1)

        @pl.when(down_ready)
        def _():
            to_partner_d(p, zt).start()

        if p == 0:

            @pl.when(i == 0)
            def _():
                share(k)

            def back(t, _):
                da = dot(dg[big(t)], wgs[slot], 1, 1) + dot(du[big(t)], wus[slot], 1, 1)
                ACC[big(t)] += da
                return 0

            lax.fori_loop(0, T // TB, back, 0)

        @pl.when(down_ready)
        def _():
            share_d(p, zt)

        @pl.when(k > 0)
        def _():
            share(k)

        @pl.when(k >= 2)
        def _():
            pass_on(k - 2)

        @pl.when(k >= 3)
        def _():
            pass_back(k - 3)

        if p == 1:

            @pl.when(i == 2)
            def _():
                for q in (3, 2):
                    for u in range(2):
                        pass_on_d(0, q, u)
                pass_back_d(0)

            @pl.when(jnp.logical_and(mid, i == 3))
            def _():
                finish_d(0)
                lax.fori_loop(0, steps, finish, 0)
                for n in range(6, 9):
                    lend(n).start()

        return 0

    lax.fori_loop(0, steps, functools.partial(backward, 0, A1), 0)

    def through_norm(t, _):
        da = ACC[rows(t)].astype(BF16).astype(F32)
        wide = H[rows(t)].astype(F32)
        scale = lax.rsqrt(jnp.mean(wide * wide, -1, keepdims=True) + 1e-6)
        along = jnp.mean(da * wide, -1, keepdims=True)
        dh = (da * scale - wide * (scale * scale * scale * along)).astype(BF16).astype(F32)
        DY[rows(t)] = (DY[rows(t)].astype(F32) + dh).astype(BF16)
        AT[:, rows(t)] = A0[rows(t)].T
        return 0

    lax.fori_loop(0, tiles, through_norm, 0)
    lax.fori_loop(0, steps, functools.partial(backward, 1, A0), 0)

    last = 2 * steps - 1
    pass_on_d(1, 3, 0)
    pass_on_d(1, 3, 1)
    pass_on(last - 1)
    pass_on_d(1, 2, 0)
    pass_on(last, True)
    pass_on_d(1, 2, 1)
    pass_back_d(1)
    pass_back(last - 2)
    pass_back(last - 1)
    pass_back(last)

    @pl.when(end)
    def _():
        finish_d(0)
        lax.fori_loop(0, steps, finish, 0)

    finish_d(1)
    lax.fori_loop(steps, 2 * steps, finish, 0)

    for n in range(9):

        @pl.when(end)
        def _():
            lend(n).wait_recv()

        @pl.when(mid)
        def _():
            lend(n).wait_send()


    def sent(k, _):
        @pl.when(end)
        def _():
            @pl.when(k < last)
            def _():
                all_from_end(k).wait_send()

            @pl.when(k == last)
            def _():
                for q in (3, 2, 1):
                    from_end(k, q).wait_send()

        @pl.when(mid)
        def _():
            across(k, 3).wait_send()
            across(k, 2).wait_send()
            to_end(k).wait_send()

        return 0

    lax.fori_loop(0, 2 * steps, sent, 0)
    for p in range(2):

        @pl.when(end)
        def _():
            for u in range(2):
                for q in (3, 2, 1):
                    from_end_d(p, q, u).wait_send()

        @pl.when(mid)
        def _():
            for u in range(2):
                across_d(p, 3, u).wait_send()
                across_d(p, 2, u).wait_send()
                to_end_d(p, u).wait_send()


def gradients(x, dy, wg, wu, wd, moments):
    T, D = x.shape
    L, _, FF = wg.shape
    n = L * (FF // CHUNK)
    RG, RD = D // 8, FF // 8
    V, DMA = pltpu.VMEM, pltpu.SemaphoreType.DMA
    piece = (2, RG, CHUNK)
    return pl.pallas_call(
        functools.partial(gradients_kernel, T, D, FF),
        out_shape=[
            V((L, RG, FF), BF16),
            V((L, RG, FF), BF16),
            V((L, RD, D), BF16),
            *(pltpu.HBM(a.shape[1:], F32) for a in moments),
            *(pltpu.HBM(a.shape[1:], BF16) for a in moments[:3]),
        ],
        in_specs=[pl.BlockSpec(memory_space=pl.ANY)] * 11,
        out_specs=[pl.BlockSpec(memory_space=pltpu.VMEM)] * 3 + [pl.BlockSpec(memory_space=pltpu.HBM)] * 9,
        scratch_shapes=[
            V((T, D), BF16), V((T, D), BF16), V((T, D), BF16), V((D, T), BF16), V((T, D), BF16), V((T, D), F32),
            V((T, CHUNK), BF16), V((T, CHUNK), BF16), V((T, CHUNK), BF16),
            V((2, D, CHUNK), BF16), V((2, D, CHUNK), BF16), V((2, CHUNK, D), BF16),
            V((4, 4, 2, *piece), BF16), V((n, 4, *piece), BF16), V((n, *piece), F32),
            V((n, 3, *piece), BF16), V((n, 2, *piece), BF16),
            V((L, FF, D), BF16), V((L, 4, RD, D), BF16), V((L, RD, D), F32),
            V((L, 3, RD, D), BF16), V((L, 2, RD, D), BF16),
            DMA((2, 3)), DMA((1,)), DMA((n,)), DMA((n,)), DMA((n, 3)), DMA((n, 3)), DMA((n,)), DMA((n, 2)),
            DMA((L, 4)), DMA((L, 4)), DMA((L, 3, 2)), DMA((L, 3, 2)), DMA((L, 2)), DMA((L, 2, 2)), DMA((9,)), DMA((9,)), DMA((T // min(512, T),)),
        ],
        compiler_params=pltpu.CompilerParams(collective_id=0, has_side_effects=True, vmem_limit_bytes=VMEM_LIMIT - 2_300_000),
        name="gradients",
    )(x, dy, wg, wu, wd, *moments)


def update_kernel(count, *refs):
    g_s, m_hbm, v_hbm, w_hbm, lent = refs[0:3], refs[3:6], refs[6:9], refs[9:12], refs[12:21]
    w_out, m_out, v_out, refs = refs[21:24], refs[24:27], refs[27:30], refs[30:]
    m_s, v_s, w_s, n_s, refs = refs[0:3], refs[3:6], refs[6:9], refs[9:12], refs[12:]
    g_n, m_n, v_n, w_n, n_n, refs = refs[0:3], refs[3:6], refs[6:9], refs[9:12], refs[12:15], refs[15:]
    sq, in_sem, sq_send, sq_recv, r_send, r_recv, l_send, l_recv, p_send, p_recv, own_sem, mv_sem, near_sem = refs
    me, z, c, h, end = placed()
    partner = z * 2 + 1 - c
    L = 2
    parts = [(l, t) for l in (0, 1) for t in (2, 0, 1)]
    inward = z + 1 - 2 * h

    loads = []
    for t in range(3):
        block = pl.ds(pl.multiple_of(me * g_s[t].shape[1], 32), g_s[t].shape[1])
        loads.append([
            pltpu.make_async_copy(m_hbm[t], m_s[t], in_sem.at[t, 0]),
            pltpu.make_async_copy(v_hbm[t], v_s[t], in_sem.at[t, 1]),
            pltpu.make_async_copy(w_hbm[t].at[:, block], w_s[t], in_sem.at[t, 2]),
        ])
    for which in range(3):
        for t in (2, 0, 1):
            loads[t][which].start()

    near = []
    for t in range(3):
        block = pl.ds(pl.multiple_of((2 * inward + c) * g_s[t].shape[1], 32), g_s[t].shape[1])
        near += [
            pltpu.make_async_copy(lent[t], m_n[t], near_sem.at[t, 0]),
            pltpu.make_async_copy(lent[3 + t], v_n[t], near_sem.at[t, 1]),
            pltpu.make_async_copy(lent[6 + t], g_n[t], near_sem.at[t, 2]),
            pltpu.make_async_copy(w_hbm[t].at[1, block], w_n[t], near_sem.at[t, 3]),
        ]

    @pl.when(end)
    def _():
        for copy in near:
            copy.start()

    barrier = pltpu.get_barrier_semaphore()
    for other in range(1, 8):
        pl.semaphore_signal(barrier, inc=1, device_id={"dp": (me + other) % 8}, device_id_type=MESH)

    STEP = 32

    def strip(r):
        return pl.ds(pl.multiple_of(r * STEP, STEP), STEP)

    total = jnp.zeros((8, 128), F32)
    for t in range(3):
        R, C = g_s[t].shape[1:]

        def squares(r, total, t=t, R=R, C=C):
            l, q = r // (R // STEP), r % (R // STEP)
            g = g_s[t][l, strip(q)].astype(F32)
            return total + jnp.sum((g * g).reshape(STEP // 8, 8, C // 128, 128), axis=(0, 2))

        total = lax.fori_loop(0, L * (R // STEP), squares, total)
    sq[me] = total
    pl.semaphore_wait(barrier, 7)

    def tell(other):
        to = (me + other) % 8
        return remote(sq.at[me], sq.at[me], sq_send.at[other], sq_recv.at[8 - other], to)

    def told(other):
        src = (me + other) % 8
        return remote(sq.at[src], sq.at[src], sq_send.at[8 - other], sq_recv.at[other], me)

    for other in range(1, 8):
        tell(other).start()
    for t in range(3):
        for which in range(3):
            loads[t][which].wait()
    for other in range(1, 8):
        told(other).wait_recv()
    for other in range(1, 8):
        tell(other).wait_send()
    whole = jnp.full((8, 128), jnp.sum(sq[...]), F32)
    factor = jnp.minimum(1.0, 0.5 * lax.rsqrt(whole / count + 1e-30))[0:1, 0:1]

    def block(p, zt, ct):
        l, t = parts[p]
        R = g_s[t].shape[1]
        return w_out[t].at[l, pl.ds(pl.multiple_of((2 * zt + ct) * R, 32), R)]

    def mine(p):
        l, t = parts[p]
        return n_s[t].at[l]

    def to_right(p, hop):
        src = mine(p) if hop == 0 else block(p, z - hop, c)
        return remote(src, block(p, z - hop, c), r_send.at[p, hop], r_recv.at[p, hop], (z + 1) * 2 + c)

    def to_left(p, hop):
        src = mine(p) if hop == 0 else block(p, z + hop, c)
        return remote(src, block(p, z + hop, c), l_send.at[p, hop], l_recv.at[p, hop], (z - 1) * 2 + c)

    def to_partner(p, zt, own=False):
        return remote(mine(p) if own else block(p, zt, c), block(p, zt, c), p_send.at[p, zt], p_recv.at[p, zt], partner)

    def keep(p):
        return pltpu.make_async_copy(mine(p), block(p, z, c), own_sem.at[p])

    def moments(p):
        l, t = parts[p]
        return (
            pltpu.make_async_copy(m_s[t].at[l], m_out[t].at[l], mv_sem.at[p, 0]),
            pltpu.make_async_copy(v_s[t].at[l], v_out[t].at[l], mv_sem.at[p, 1]),
        )

    def adamw(g, m, v, w):
        g, w = g.astype(F32) * factor, w.astype(F32)
        m = 0.9 * m + 0.1 * g
        v = 0.95 * v + 0.05 * g * g
        return (w - 0.02 * (m * lax.rsqrt(v + 1e-8) + 0.1 * w)).astype(BF16), m, v

    def sends_right(p, hop):
        if hop == 0 and parts[p][0] == 1:
            return jnp.logical_and(z < 3, z != 2)
        return jnp.logical_and(z < 3, z >= hop)

    def sends_left(p, hop):
        if hop == 0 and parts[p][0] == 1:
            return jnp.logical_and(z > 0, z != 1)
        return jnp.logical_and(z > 0, z + hop <= 3)

    for p, (l, t) in enumerate(parts):

        def own(r, _, l=l, t=t):
            at = strip(r)
            new, m, v = adamw(g_s[t][l, at], m_s[t][l, at], v_s[t][l, at], w_s[t][l, at])
            m_s[t][l, at] = m
            v_s[t][l, at] = v
            n_s[t][l, at] = new
            return 0

        lax.fori_loop(0, g_s[t].shape[1] // STEP, own, 0)

        @pl.when(sends_right(p, 0))
        def _():
            to_right(p, 0).start()

        @pl.when(sends_left(p, 0))
        def _():
            to_left(p, 0).start()

        to_partner(p, z, True).start()
        keep(p).start()
        for copy in moments(p):
            copy.start()

    def near_block(p):
        return block(p, inward, c)

    def near_keep(p):
        return pltpu.make_async_copy(n_n[parts[p][1]], near_block(p), own_sem.at[p])

    def near_to_partner(p):
        return remote(n_n[parts[p][1]], near_block(p), p_send.at[p, inward], p_recv.at[p, inward], partner)

    @pl.when(end)
    def _():
        for copy in near:
            copy.wait()
        for p, (l, t) in enumerate(parts):
            if l == 1:

                def neighbour(r, _, t=t):
                    at = strip(r)
                    n_n[t][at] = adamw(g_n[t][at], m_n[t][at], v_n[t][at], w_n[t][at])[0]
                    return 0

                lax.fori_loop(0, g_s[t].shape[1] // STEP, neighbour, 0)
                near_to_partner(p).start()
                keep(p).wait()
                near_keep(p).start()

    n = len(parts)
    for hop in range(3):
        for p in range(n):
            borrowed = hop == 0 and parts[p][0] == 1

            @pl.when(jnp.logical_and(z > hop, z != 3) if borrowed else z > hop)
            def _():
                to_right(p, hop).wait_recv()

                if hop < 2:

                    @pl.when(z < 3)
                    def _():
                        to_right(p, hop + 1).start()

                to_partner(p, z - hop - 1).start()

            @pl.when(jnp.logical_and(z + hop < 3, z != 0) if borrowed else z + hop < 3)
            def _():
                to_left(p, hop).wait_recv()

                if hop < 2:

                    @pl.when(z > 0)
                    def _():
                        to_left(p, hop + 1).start()

                to_partner(p, z + hop + 1).start()

    for p in range(n):
        for zt in range(4):
            to_partner(p, zt).wait_recv()
    for p in range(n):
        keep(p).wait()
        for copy in moments(p):
            copy.wait()
        for zt in range(4):
            to_partner(p, zt).wait_send()
        for hop in range(3):

            @pl.when(sends_right(p, hop))
            def _():
                to_right(p, hop).wait_send()

            @pl.when(sends_left(p, hop))
            def _():
                to_left(p, hop).wait_send()


def update(g, m, v, w, lent):
    V, DMA = pltpu.VMEM, pltpu.SemaphoreType.DMA
    S = jax.ShapeDtypeStruct
    count = 8 * sum(a.size for a in g)
    out = [V(a.shape, BF16) for a in w] + [V(a.shape, F32) for a in (*m, *v)]
    return pl.pallas_call(
        functools.partial(update_kernel, float(count)),
        out_shape=out,
        in_specs=[pl.BlockSpec(memory_space=pltpu.VMEM)] * 3 + [pl.BlockSpec(memory_space=pltpu.HBM)] * 18,
        out_specs=[pl.BlockSpec(memory_space=pl.ANY)] * 9,
        scratch_shapes=[
            *(V(a.shape, F32) for a in m), *(V(a.shape, F32) for a in v),
            *(V(a.shape, BF16) for a in g), *(V(a.shape, BF16) for a in g),
            *(V(a.shape[1:], BF16) for a in g), *(V(a.shape[1:], F32) for a in m), *(V(a.shape[1:], F32) for a in v),
            *(V(a.shape[1:], BF16) for a in g), *(V(a.shape[1:], BF16) for a in g),
            V((8, 8, 128), F32), DMA((3, 3)), DMA((8,)), DMA((8,)),
            DMA((6, 3)), DMA((6, 3)), DMA((6, 3)), DMA((6, 3)), DMA((6, 4)), DMA((6, 4)), DMA((6,)), DMA((6, 2)), DMA((3, 4)),
        ],
        compiler_params=pltpu.CompilerParams(collective_id=1, has_side_effects=True, vmem_limit_bytes=36_000_000),
        name="update",
    )(*(pltpu.with_memory_space_constraint(a, pltpu.VMEM) for a in g), *m, *v, *w, *lent)


def store_kernel(*refs):
    n = len(refs) // 2
    src, dst, sem = refs[:n], refs[n : 2 * n], refs[2 * n]
    copies = [pltpu.make_async_copy(src[i].at[l], dst[i].at[l], sem.at[i, l]) for i in range(n) for l in range(2)]
    for copy in copies:
        copy.start()
    for copy in copies:
        copy.wait()


def store(arrays):
    n = len(arrays)
    return pl.pallas_call(
        store_kernel,
        out_shape=[jax.ShapeDtypeStruct(a.shape, a.dtype) for a in arrays],
        in_specs=[pl.BlockSpec(memory_space=pl.ANY)] * n,
        out_specs=[pl.BlockSpec(memory_space=pltpu.HBM)] * n,
        scratch_shapes=[pltpu.SemaphoreType.DMA((n, 2))],
        compiler_params=pltpu.CompilerParams(vmem_limit_bytes=1_000_000),
        name="store",
    )(*arrays)


def solution(mesh):
    def step(x, dy, *arrays):
        w, m, v = (arrays[i : i + 3] for i in (0, 3, 6))
        out = gradients(x[0], dy[0], *w, (*m, *v))
        return tuple(store(update(out[:3], m, v, w, out[3:])))

    whole, split = P(None, None, None), P(None, "dp", None)
    return jax.shard_map(
        step,
        mesh=mesh,
        in_specs=(P(("rep", "dp")),) * 2 + (whole,) * 3 + (split,) * 6,
        out_specs=(P("rep", None, None),) * 3 + (P("rep", "dp", None),) * 6,
        check_vma=False,
    )
```
